32 devices in a mesh: batch: 2 (over x), col: 4 (over z), row: 4 (over y, core).
Axes of the slice: x: 2, y: 2, z: 4, core: 2. Of those that a mesh axis runs over, the one named last changes fastest.
Arguments:
- pair_rep: bfloat16 [1536, 768, 64], P(('batch', 'row'), 'col'), parts along dimension 0
- pair_mask: int32 [1536, 768], P(('batch', 'row'), 'col'), parts along dimension 0
- ln_in_scale: bfloat16 [64], replicated
- w_left: bfloat16 [64, 64], replicated
- w_left_gate: bfloat16 [64, 64], replicated
- w_right: bfloat16 [64, 64], replicated
- w_right_gate: bfloat16 [64, 64], replicated
- w_out_gate: bfloat16 [64, 64], replicated
- ln_out_scale: bfloat16 [64], replicated
- w_out: bfloat16 [64, 64], replicated
Outputs:
- output: bfloat16 [1536, 768, 64], P(('batch', 'row'), 'col'), parts along dimension 0
There are 2 independent parts. The reference program is written for one: setup_inputs(seed, part) draws one part's arguments, and reference() takes and returns one part's arrays. A program takes and returns all parts, laid end to end along the dimension named above; an argument that names none is the same for every part.
All inputs are finite; a program needn't handle non-finite values.
Results may differ from the reference program's by a relative error of at most 0.001.
Values are sent between devices in bfloat16 or wider.
A program may use at most 1 GiB of HBM per device.

```python
import math
import jax
import jax.numpy as jnp
from jax import lax

RESIDUES = 768
PAIR_DIM = 64
TRI_DIM = 64
ROW_BLK = math.gcd(RESIDUES, 64)
NUM_BLK = RESIDUES // ROW_BLK
LN_EPS = 0.00001


def layer_norm(values, gain_vec):
    mean_val = jnp.mean(values, axis=-1, keepdims=True)
    centered = values - mean_val
    variance = jnp.mean(centered * centered, axis=-1, keepdims=True)
    return centered * lax.rsqrt(variance + LN_EPS) * gain_vec.astype(jnp.float32)


def setup_inputs(seed: int = 0, part: int = 0) -> dict:
    part_keys = jax.random.split(jax.random.fold_in(jax.random.key(seed), part), 3)
    weight_keys = jax.random.split(jax.random.key(seed + 1), 8)
    pair_rep = jax.random.normal(part_keys[0], (RESIDUES, RESIDUES, PAIR_DIM), jnp.float32).astype(jnp.bfloat16)
    residue_ok = jax.random.randint(part_keys[1], (RESIDUES,), 0, 16) != 0
    pair_ok = jax.random.randint(part_keys[2], (RESIDUES, RESIDUES), 0, 8) != 0
    pair_mask = (residue_ok[:, None] & residue_ok[None, :] & pair_ok).astype(jnp.int32)

    def matrix(key_val, fan_in, fan_out):
        return (jax.random.normal(key_val, (fan_in, fan_out), jnp.float32) * fan_in ** -0.5).astype(jnp.bfloat16)

    def gain_vector(key_val, num_chan):
        return (1.0 + 0.5 * jax.random.normal(key_val, (num_chan,), jnp.float32)).astype(jnp.bfloat16)

    return {
        'pair_rep': pair_rep,
        'pair_mask': pair_mask,
        'ln_in_scale': gain_vector(weight_keys[0], PAIR_DIM),
        'w_left': matrix(weight_keys[1], PAIR_DIM, TRI_DIM),
        'w_left_gate': matrix(weight_keys[2], PAIR_DIM, TRI_DIM),
        'w_right': matrix(weight_keys[3], PAIR_DIM, TRI_DIM),
        'w_right_gate': matrix(weight_keys[4], PAIR_DIM, TRI_DIM),
        'w_out_gate': matrix(weight_keys[5], PAIR_DIM, PAIR_DIM),
        'ln_out_scale': gain_vector(weight_keys[6], TRI_DIM),
        'w_out': matrix(weight_keys[7], TRI_DIM, PAIR_DIM),
    }


def reference(pair_rep, pair_mask, ln_in_scale, w_left, w_left_gate, w_right, w_right_gate, w_out_gate, ln_out_scale, w_out):
    pair_blocks = pair_rep.reshape(NUM_BLK, ROW_BLK, RESIDUES, PAIR_DIM)
    mask_blocks = pair_mask.reshape(NUM_BLK, ROW_BLK * RESIDUES, 1).astype(jnp.float32)

    def project(block_args):
        pair_rows, keep_rows = block_args
        normed = layer_norm(pair_rows.astype(jnp.float32), ln_in_scale).astype(jnp.bfloat16).reshape(ROW_BLK * RESIDUES, PAIR_DIM)
        left_act = keep_rows * jax.nn.sigmoid(jnp.dot(normed, w_left_gate, preferred_element_type=jnp.float32)) * jnp.dot(normed, w_left, preferred_element_type=jnp.float32)
        right_act = keep_rows * jax.nn.sigmoid(jnp.dot(normed, w_right_gate, preferred_element_type=jnp.float32)) * jnp.dot(normed, w_right, preferred_element_type=jnp.float32)
        return left_act.astype(jnp.bfloat16), right_act.astype(jnp.bfloat16)

    left_all, right_all = lax.map(project, (pair_blocks, mask_blocks))
    right_t = right_all.reshape(RESIDUES, RESIDUES, TRI_DIM).astype(jnp.float32).transpose(2, 0, 1)
    left_blocks = left_all.reshape(RESIDUES, NUM_BLK, ROW_BLK, TRI_DIM).transpose(1, 3, 0, 2)

    def finish(block_args):
        left_cols, pair_rows = block_args
        summed = jnp.einsum('hki,hkj->ijh', left_cols.astype(jnp.float32), right_t)
        normed_out = layer_norm(summed, ln_out_scale).astype(jnp.bfloat16).reshape(ROW_BLK * RESIDUES, TRI_DIM)
        update = jnp.dot(normed_out, w_out, preferred_element_type=jnp.float32)
        pair_flat = pair_rows.astype(jnp.float32).reshape(ROW_BLK * RESIDUES, PAIR_DIM)
        normed_in = layer_norm(pair_flat, ln_in_scale).astype(jnp.bfloat16)
        gate_act = jax.nn.sigmoid(jnp.dot(normed_in, w_out_gate, preferred_element_type=jnp.float32))
        return (pair_flat + gate_act * update).astype(jnp.bfloat16).reshape(ROW_BLK, RESIDUES, PAIR_DIM)

    return lax.map(finish, (left_blocks, pair_blocks)).reshape(RESIDUES, RESIDUES, PAIR_DIM)
```

```python
import jax
import jax.numpy as jnp
from jax import lax
from jax.experimental import pallas as pl
from jax.experimental.pallas import tpu as pltpu
from jax.sharding import PartitionSpec as P

LN_EPS = 0.00001
MESH = pl.DeviceIdType.MESH
CHUNKS = 8


def sigmoid(v):
    return 0.5 * jnp.tanh(0.5 * v) + 0.5


def norm_channels(v, gain, axis):
    mean = jnp.mean(v, axis=axis, keepdims=True)
    cen = v - mean
    var = jnp.mean(cen * cen, axis=axis, keepdims=True)
    return cen * lax.rsqrt(var + LN_EPS) * gain


def project_kernel(z_ref, m_ref, gin_ref, we_ref, wo_ref, a_ref, b_ref):
    gain = gin_ref[...][None]
    for half in range(2):
        z = z_ref[16 * half:16 * half + 16].astype(jnp.float32)
        x = norm_channels(z, gain, 1).astype(jnp.bfloat16).reshape(4, 256, 192)
        m = m_ref[16 * half:16 * half + 16].astype(jnp.float32)

        def lanes(p, q):
            return jnp.concatenate([p[:, :128], q[:, :128], p[:, 128:], q[:, 128:]], axis=1)

        acts = []
        for par, w_ref in ((0, we_ref), (1, wo_ref)):
            rhs = lanes(x[par], x[par + 2])
            keep = lanes(m[4 * par:4 * par + 4], m[4 * par + 8:4 * par + 12])
            keep = jnp.concatenate([keep, keep], axis=0)[None]
            proj = jnp.dot(w_ref[...], rhs, preferred_element_type=jnp.float32)
            proj = proj.reshape(4, 32, 8, 384)
            acts.append((keep * sigmoid(proj[1]) * proj[0], keep * sigmoid(proj[3]) * proj[2]))
        low = lax.broadcasted_iota(jnp.int32, (32, 8, 384), 1) < 4
        for e, o, ref in ((acts[0][0], acts[1][0], a_ref), (acts[0][1], acts[1][1], b_ref)):
            first = jnp.where(low, e, o)
            second = jnp.where(low, o, e)
            both = jnp.stack([first, second], axis=1).reshape(64, 8, 384).astype(jnp.bfloat16)
            for sec in range(3):
                ref[:, sec, 8 * half:8 * half + 8, :] = both[:, :, 128 * sec:128 * sec + 128]


def project(z, m, gin, w_even, w_odd):
    full = lambda i: (0, 0)
    tile = jax.ShapeDtypeStruct((64, 3, 96, 128), jnp.bfloat16)
    out_spec = pl.BlockSpec((64, 3, 16, 128), lambda i: (0, 0, i, 0))
    return pl.pallas_call(
        project_kernel,
        grid=(6,),
        out_shape=[tile, tile],
        in_specs=[
            pl.BlockSpec((32, 64, 192), lambda i: (i, 0, 0)),
            pl.BlockSpec((32, 192), lambda i: (i, 0)),
            pl.BlockSpec((64, 1), full),
            pl.BlockSpec((1024, 256), full),
            pl.BlockSpec((1024, 256), full),
        ],
        out_specs=[out_spec, out_spec],
        compiler_params=pltpu.CompilerParams(vmem_limit_bytes=48 * 1024 * 1024),
    )(z, m, gin, w_even, w_odd)


def move_kernel(a_ref, b_ref, pa, pb, tr, stage_a, stage_b, sem_a, sem_b, sem_tr, snd, loc):
    bat, z, row = lax.axis_index('batch'), lax.axis_index('col'), lax.axis_index('row')
    y, core = row // 2, row % 2
    size = 64 // CHUNKS

    def flip(v, n, fam):
        return jnp.where(fam == 0, v, n - v)

    def dev(col, r):
        return {'batch': bat, 'col': col, 'row': r}

    def rc(src, dst, send, recv, col, r):
        return pltpu.make_async_remote_copy(
            src_ref=src, dst_ref=dst, send_sem=send, recv_sem=recv, device_id=dev(col, r), device_id_type=MESH)

    def part(ref, c):
        return ref.at[pl.ds(c * size, size)]

    def slot(ref, s, c):
        return ref.at[s, pl.ds(c * size, size)]

    fam = z // 2
    blk = flip(z, 3, fam)
    home = y == fam
    k_src = flip(row, 3, fam)

    def to_home(c):
        return rc(part(a_ref, c), slot(pa, row, c), snd.at[0, c], sem_a.at[row, c], z, z)

    def to_transit(c):
        return rc(part(a_ref, c), slot(tr, blk, c), snd.at[1, c], sem_tr.at[blk, c], flip(k_src, 3, fam), row)

    def b_far(c):
        return rc(part(b_ref, c), slot(pb, row, c), snd.at[2, c], sem_b.at[row, c], z, 2 * (1 - y) + core)

    def b_near(c):
        return rc(part(b_ref, c), slot(pb, row, c), snd.at[3, c], sem_b.at[row, c], z, 2 * y + 1 - core)

    far_row = 2 * (1 - y) + core

    def b_relay(c):
        return rc(slot(pb, far_row, c), slot(pb, far_row, c), snd.at[4, c], sem_b.at[far_row, c], z, 2 * y + 1 - core)

    zz, ii = flip(z, 3, y), flip(row, 3, y)

    def real(kk):
        return flip(jnp.int32(kk), 3, y)

    def right(kk, c):
        k = real(kk)
        return rc(slot(pa, k, c), slot(pa, k, c), snd.at[5 + kk, c], sem_a.at[k, c], jnp.where(y == 0, z + 1, z - 1), row)

    def left(kk, c):
        k = real(kk)
        return rc(slot(pa, k, c), slot(pa, k, c), snd.at[9 + kk, c], sem_a.at[k, c], jnp.where(y == 0, z - 1, z + 1), row)

    ofam = 1 - y
    oz, ok = flip(z, 3, ofam), flip(row, 3, ofam)
    is_way = (oz >= 2) & (ok == oz)

    def up(i2, c):
        return rc(slot(tr, i2, c), slot(pa, row, c), snd.at[13 + i2, c], sem_a.at[row, c], z, flip(jnp.int32(i2), 3, ofam))

    is_src = (ii == zz)
    own_home = home & (row == z)

    cp_a = pltpu.make_async_copy(a_ref, stage_a, loc.at[0])
    cp_b = pltpu.make_async_copy(b_ref, stage_b, loc.at[1])

    @pl.when(own_home)
    def _():
        cp_a.start()

    cp_b.start()

    def for_chunks(f):
        def body(c, _):
            f(c)
            return 0
        lax.fori_loop(0, CHUNKS, body, 0)

    def first_sends(c):
        @pl.when(jnp.logical_not(own_home))
        def _():
            to_home(c).start()

        @pl.when(jnp.logical_not(home))
        def _():
            to_transit(c).start()

    for_chunks(first_sends)

    def b_sends(c):
        b_far(c).start()
        b_near(c).start()

    for_chunks(b_sends)

    @pl.when(own_home)
    def _():
        cp_a.wait()
        out = pltpu.make_async_copy(stage_a, pa.at[row], loc.at[2])
        out.start()
        out.wait()

    cp_b.wait()
    out_b = pltpu.make_async_copy(stage_b, pb.at[row], loc.at[3])
    out_b.start()

    def wait_a(kk, c):
        k = real(kk)

        @pl.when(jnp.logical_not(own_home & (k == row)))
        def _():
            rc(slot(pa, k, c), slot(pa, k, c), snd.at[0, c], sem_a.at[k, c], z, row).wait_recv()

    goes_right = [
        ((zz == 0) & is_src) | ((zz == 1)) | (zz == 2),
        ((zz == 0) & is_src) | ((zz == 1)) | (zz == 2),
        ((zz == 0) & is_src) | (zz == 2),
        ((zz == 0) & is_src),
    ]
    goes_left = [
        (zz == 1) & is_src,
        (zz == 1) & is_src,
        (zz == 1) & is_src,
        ((zz == 1) & is_src) | (zz == 3),
    ]

    def relay(c):
        for kk in range(4):
            wait_a(kk, c)

            @pl.when(goes_right[kk])
            def _():
                right(kk, c).start()

            @pl.when(goes_left[kk])
            def _():
                left(kk, c).start()
            if kk == 1:
                @pl.when(is_way)
                def _():
                    for i2 in range(2):
                        rc(slot(tr, i2, c), slot(tr, i2, c), snd.at[0, c], sem_tr.at[i2, c], z, row).wait_recv()
                        up(i2, c).start()

    for_chunks(relay)

    def b_relays(c):
        rc(slot(pb, far_row, c), slot(pb, far_row, c), snd.at[0, c], sem_b.at[far_row, c], z, row).wait_recv()
        b_relay(c).start()

    for_chunks(b_relays)

    def drain(c):
        for r in (2 * y + 1 - core, 2 * (1 - y) + 1 - core):
            rc(slot(pb, r, c), slot(pb, r, c), snd.at[0, c], sem_b.at[r, c], z, row).wait_recv()

        @pl.when(jnp.logical_not(own_home))
        def _():
            to_home(c).wait_send()

        @pl.when(jnp.logical_not(home))
        def _():
            to_transit(c).wait_send()
        b_far(c).wait_send()
        b_near(c).wait_send()
        b_relay(c).wait_send()
        for kk in range(4):
            @pl.when(goes_right[kk])
            def _():
                right(kk, c).wait_send()

            @pl.when(goes_left[kk])
            def _():
                left(kk, c).wait_send()

        @pl.when(is_way)
        def _():
            for i2 in range(2):
                up(i2, c).wait_send()

    for_chunks(drain)
    out_b.wait()


def move(a, b):
    tile = (64, 3, 96, 128)
    any_spec = pl.BlockSpec(memory_space=pltpu.HBM)
    pa, pb, _ = pl.pallas_call(
        move_kernel,
        out_shape=[jax.ShapeDtypeStruct((n,) + tile, jnp.bfloat16) for n in (4, 4, 2)],
        in_specs=[any_spec] * 2,
        out_specs=[any_spec] * 3,
        scratch_shapes=[
            pltpu.VMEM(tile, jnp.bfloat16),
            pltpu.VMEM(tile, jnp.bfloat16),
            pltpu.SemaphoreType.DMA((4, CHUNKS)),
            pltpu.SemaphoreType.DMA((4, CHUNKS)),
            pltpu.SemaphoreType.DMA((2, CHUNKS)),
            pltpu.SemaphoreType.DMA((15, CHUNKS)),
            pltpu.SemaphoreType.DMA((4,)),
        ],
        compiler_params=pltpu.CompilerParams(has_side_effects=True),
    )(a, b)
    return pa, pb


H_STEP = 4
E_STEPS = 64 // H_STEP
I_STEP = 16


def finish_kernel(pa_ref, pb_ref, z_ref, gin_ref, gout_ref, wg_ref, wo_ref, out_ref, o_ref):
    step = pl.program_id(0)

    @pl.when(step < E_STEPS)
    def _():
        def one(h, _):
            def sides(ref):
                sec = [ref[:, h, s].reshape(384, 128) for s in range(3)]
                return jnp.concatenate([sec[0], sec[2]], axis=1), jnp.concatenate([sec[1], sec[2]], axis=1)

            a_lo, a_hi = sides(pa_ref)
            b_lo, b_hi = sides(pb_ref)
            dims = (((0,), (0,)), ((), ()))
            lo = lax.dot_general(a_lo, b_lo, dims, preferred_element_type=jnp.float32)
            hi = lax.dot_general(a_hi, b_hi, dims, preferred_element_type=jnp.float32)
            hh = step * H_STEP + h
            o_ref[hh, 0:128, 0:128] = lo[0:128, 0:128] + hi[0:128, 0:128]
            o_ref[hh, 128:192, 0:128] = lo[128:192, 0:128] + hi[192:256, 0:128]
            right = jnp.concatenate(
                [lo[0:128, 128:192] + hi[0:128, 192:256], lo[128:192, 128:192] + lo[192:256, 192:256]], axis=0)
            o_ref[hh, :, 128:192] = right
            return 0

        lax.fori_loop(0, H_STEP, one, 0)

    @pl.when(step >= E_STEPS)
    def _():
        base = (step - E_STEPS) * I_STEP
        for q in range(I_STEP // 8):
            rows = pl.ds(pl.multiple_of(base + 8 * q, 8), 8)
            o = o_ref[:, rows, :]
            yv = norm_channels(o, gout_ref[...], 0).astype(jnp.bfloat16).reshape(512, 192)
            upd = jnp.dot(wo_ref[...], yv, preferred_element_type=jnp.float32)
            zv = z_ref[8 * q:8 * q + 8].astype(jnp.float32)
            x = norm_channels(zv, gin_ref[...][None], 1).astype(jnp.bfloat16).reshape(2, 256, 192)
            for s in range(2):
                gate = sigmoid(jnp.dot(wg_ref[...], x[s], preferred_element_type=jnp.float32))
                res = zv[4 * s:4 * s + 4].reshape(256, 192) + gate * upd[256 * s:256 * s + 256]
                out_ref[8 * q + 4 * s:8 * q + 4 * s + 4] = res.astype(jnp.bfloat16).reshape(4, 64, 192)


def finish(pa, pb, z, gin, gout, wg, wo):
    panel = pl.BlockSpec((4, H_STEP, 3, 96, 128), lambda i: (0, jnp.minimum(i, E_STEPS - 1), 0, 0, 0))
    rows = pl.BlockSpec((I_STEP, 64, 192), lambda i: (jnp.maximum(i - E_STEPS, 0), 0, 0))
    full2 = lambda i: (0, 0)
    return pl.pallas_call(
        finish_kernel,
        grid=(E_STEPS + 192 // I_STEP,),
        out_shape=jax.ShapeDtypeStruct((192, 64, 192), jnp.bfloat16),
        in_specs=[
            panel, panel, rows,
            pl.BlockSpec((64, 1), full2),
            pl.BlockSpec((64, 1, 1), lambda i: (0, 0, 0)),
            pl.BlockSpec((256, 256), full2),
            pl.BlockSpec((512, 512), full2),
        ],
        out_specs=rows,
        scratch_shapes=[pltpu.VMEM((64, 192, 192), jnp.float32)],
        compiler_params=pltpu.CompilerParams(vmem_limit_bytes=48 * 1024 * 1024),
    )(pa, pb, z, gin, gout, wg, wo)


def spread(w, n, swap=False):
    t = w.T
    if swap:
        t = t.reshape(32, 2, 64)[:, ::-1].reshape(64, 64)
    eye = jnp.eye(n, dtype=w.dtype)
    return (t[:, None, None, :] * eye[None, :, :, None]).reshape(64 * n, 64 * n)


def solution(mesh):
    tile_spec = P(('batch', 'row'), 'col', None)
    mask_spec = P(('batch', 'row'), 'col')
    replicated = P()

    def local_step(pair, mask, gin, w_l, w_lg, w_r, w_rg, w_g, gout, w_o):
        z = jnp.transpose(pair, (0, 2, 1))
        gin_c = gin.astype(jnp.float32)[:, None]
        gout_c = gout.astype(jnp.float32)[:, None, None]
        w_even = jnp.concatenate([spread(w, 4) for w in (w_l, w_lg, w_r, w_rg)], axis=0)
        w_odd = jnp.concatenate([spread(w, 4, True) for w in (w_l, w_lg, w_r, w_rg)], axis=0)
        eye4, eye8 = jnp.eye(4, dtype=w_g.dtype), jnp.eye(8, dtype=w_o.dtype)
        wg4 = (eye4[:, None, :, None] * w_g.T[None, :, None, :]).reshape(256, 256)
        wo8 = (eye8[:, None, None, :] * w_o.T[None, :, :, None]).reshape(512, 512)
        a, b = project(z, mask, gin_c, w_even, w_odd)
        pa, pb = move(a, b)
        out = finish(pa, pb, z, gin_c, gout_c, wg4, wo8)
        return jnp.transpose(out, (0, 2, 1))

    return jax.shard_map(local_step, mesh=mesh, in_specs=(tile_spec, mask_spec) + (replicated,) * 8, out_specs=tile_spec, check_vma=False)
```

```python
import jax
import jax.numpy as jnp
from jax import lax
from jax.experimental import pallas as pl
from jax.experimental.pallas import tpu as pltpu
from jax.sharding import PartitionSpec as P

LN_EPS = 0.00001
MESH = pl.DeviceIdType.MESH
CHUNKS = 16
WAY_LAG = 5
FAR_LAG = 10


def sigmoid(v):
    return 0.5 * jnp.tanh(0.5 * v) + 0.5


def norm_channels(v, gain, axis):
    mean = jnp.mean(v, axis=axis, keepdims=True)
    cen = v - mean
    var = jnp.mean(cen * cen, axis=axis, keepdims=True)
    return cen * lax.rsqrt(var + LN_EPS) * gain


def project_kernel(z_ref, m_ref, gin_ref, we_ref, wo_ref, a_ref, b_ref):
    gain = gin_ref[...][None]
    for half in range(2):
        z = z_ref[16 * half:16 * half + 16].astype(jnp.float32)
        x = norm_channels(z, gain, 1).astype(jnp.bfloat16).reshape(4, 256, 192)
        m = m_ref[16 * half:16 * half + 16].astype(jnp.float32)

        def lanes(p, q):
            return jnp.concatenate([p[:, :128], q[:, :128], p[:, 128:], q[:, 128:]], axis=1)

        acts = []
        for par, w_ref in ((0, we_ref), (1, wo_ref)):
            rhs = lanes(x[par], x[par + 2])
            keep = lanes(m[4 * par:4 * par + 4], m[4 * par + 8:4 * par + 12])
            keep = jnp.concatenate([keep, keep], axis=0)[None]
            proj = jnp.dot(w_ref[...], rhs, preferred_element_type=jnp.float32)
            proj = proj.reshape(4, 32, 8, 384)
            acts.append((keep * sigmoid(proj[1]) * proj[0], keep * sigmoid(proj[3]) * proj[2]))
        low = lax.broadcasted_iota(jnp.int32, (32, 8, 384), 1) < 4
        for e, o, ref in ((acts[0][0], acts[1][0], a_ref), (acts[0][1], acts[1][1], b_ref)):
            first = jnp.where(low, e, o)
            second = jnp.where(low, o, e)
            both = jnp.stack([first, second], axis=1).reshape(64, 8, 384).astype(jnp.bfloat16)
            for sec in range(3):
                ref[:, sec, 8 * half:8 * half + 8, :] = both[:, :, 128 * sec:128 * sec + 128]


def project(z, m, gin, w_even, w_odd):
    full = lambda i: (0, 0)
    tile = jax.ShapeDtypeStruct((64, 3, 96, 128), jnp.bfloat16)
    out_spec = pl.BlockSpec((64, 3, 16, 128), lambda i: (0, 0, i, 0))
    return pl.pallas_call(
        project_kernel,
        grid=(6,),
        out_shape=[tile, tile],
        in_specs=[
            pl.BlockSpec((32, 64, 192), lambda i: (i, 0, 0)),
            pl.BlockSpec((32, 192), lambda i: (i, 0)),
            pl.BlockSpec((64, 1), full),
            pl.BlockSpec((1024, 256), full),
            pl.BlockSpec((1024, 256), full),
        ],
        out_specs=[out_spec, out_spec],
        compiler_params=pltpu.CompilerParams(vmem_limit_bytes=48 * 1024 * 1024),
    )(z, m, gin, w_even, w_odd)


def move_kernel(a_ref, b_ref, pa, pb, tr, stage_a, stage_b, sem_a, sem_b, sem_tr, snd, loc):
    bat, z, row = lax.axis_index('batch'), lax.axis_index('col'), lax.axis_index('row')
    y, core = row // 2, row % 2
    size = 64 // CHUNKS

    def flip(v, n, fam):
        return jnp.where(fam == 0, v, n - v)

    def dev(col, r):
        return {'batch': bat, 'col': col, 'row': r}

    def rc(src, dst, send, recv, col, r):
        return pltpu.make_async_remote_copy(
            src_ref=src, dst_ref=dst, send_sem=send, recv_sem=recv, device_id=dev(col, r), device_id_type=MESH)

    def part(ref, c):
        return ref.at[pl.ds(c * size, size)]

    def slot(ref, s, c):
        return ref.at[s, pl.ds(c * size, size)]

    fam = z // 2
    blk = flip(z, 3, fam)
    home = y == fam
    k_src = flip(row, 3, fam)

    def to_home(c):
        return rc(part(a_ref, c), slot(pa, row, c), snd.at[0, c], sem_a.at[row, c], z, z)

    def to_transit(c):
        return rc(part(a_ref, c), slot(tr, blk, c), snd.at[1, c], sem_tr.at[blk, c], flip(k_src, 3, fam), flip(5 - k_src, 3, fam))

    def b_far(c):
        return rc(part(b_ref, c), slot(pb, row, c), snd.at[2, c], sem_b.at[row, c], z, 2 * (1 - y) + core)

    def b_near(c):
        return rc(part(b_ref, c), slot(pb, row, c), snd.at[3, c], sem_b.at[row, c], z, 2 * y + 1 - core)

    far_row = 2 * (1 - y) + core

    def b_relay(c):
        return rc(slot(pb, far_row, c), slot(pb, far_row, c), snd.at[4, c], sem_b.at[far_row, c], z, 2 * y + 1 - core)

    zz, ii = flip(z, 3, y), flip(row, 3, y)

    def real(kk):
        return flip(jnp.int32(kk), 3, y)

    def right(kk, c):
        k = real(kk)
        return rc(slot(pa, k, c), slot(pa, k, c), snd.at[5 + kk, c], sem_a.at[k, c], jnp.where(y == 0, z + 1, z - 1), row)

    def left(kk, c):
        k = real(kk)
        return rc(slot(pa, k, c), slot(pa, k, c), snd.at[9 + kk, c], sem_a.at[k, c], jnp.where(y == 0, z - 1, z + 1), row)

    ofam = 1 - y
    oz, ok = flip(z, 3, ofam), flip(row, 3, ofam)
    is_way = (oz >= 2) & (ok == 5 - oz)
    way_k = flip(oz, 3, ofam)

    def up(i2, c):
        return rc(slot(tr, i2, c), slot(pa, way_k, c), snd.at[13 + i2, c], sem_a.at[way_k, c], z, flip(jnp.int32(i2), 3, ofam))

    is_src = (ii == zz)
    own_home = home & (row == z)

    cp_a = pltpu.make_async_copy(a_ref, stage_a, loc.at[0])
    cp_b = pltpu.make_async_copy(b_ref, stage_b, loc.at[1])

    @pl.when(own_home)
    def _():
        cp_a.start()

    cp_b.start()

    def for_chunks(f):
        def body(c, _):
            f(c)
            return 0
        lax.fori_loop(0, CHUNKS, body, 0)

    def first_sends(c):
        @pl.when(jnp.logical_not(own_home))
        def _():
            to_home(c).start()

        @pl.when(jnp.logical_not(home))
        def _():
            to_transit(c).start()

    for_chunks(first_sends)

    @pl.when(own_home)
    def _():
        cp_a.wait()
        out = pltpu.make_async_copy(stage_a, pa.at[row], loc.at[2])
        out.start()
        out.wait()

    cp_b.wait()
    out_b = pltpu.make_async_copy(stage_b, pb.at[row], loc.at[3])
    out_b.start()

    def wait_a(kk, c):
        k = real(kk)

        @pl.when(jnp.logical_not(own_home & (k == row)))
        def _():
            rc(slot(pa, k, c), slot(pa, k, c), snd.at[0, c], sem_a.at[k, c], z, row).wait_recv()

    goes_right = [
        ((zz == 0) & is_src) | ((zz == 1)) | (zz == 2),
        ((zz == 0) & is_src) | ((zz == 1)) | (zz == 2),
        ((zz == 0) & is_src) | (zz == 2),
        ((zz == 0) & is_src),
    ]
    goes_left = [
        (zz == 1) & is_src,
        (zz == 1) & is_src,
        (zz == 1) & is_src,
        ((zz == 1) & is_src) | (zz == 3),
    ]

    def wait_slot(ref, sem, s, c):
        rc(slot(ref, s, c), slot(ref, s, c), snd.at[0, c], sem.at[s, c], z, row).wait_recv()

    goes = [goes_right[kk] | goes_left[kk] for kk in range(4)]
    near_lag = [0, 0, 1, 1]
    forwards = []
    for kk in range(4):
        forwards.append((near_lag[kk], kk, goes[kk] & (zz < 2) & is_src))
    for kk in range(2):
        forwards.append((1, kk, (zz == 1) & jnp.logical_not(is_src)))
        forwards.append((2, kk, zz == 2))
    forwards.append((FAR_LAG, 2, zz == 2))
    forwards.append((FAR_LAG, 3, zz == 3))
    forwards.sort(key=lambda f: f[0])

    def in_range(s, lag):
        return (s >= lag) & (s < CHUNKS + lag)

    def relay(s, _):
        @pl.when(s < CHUNKS)
        def _():
            b_far(s).start()
            b_near(s).start()

        for lag, kk, who in forwards:
            @pl.when(in_range(s, lag) & who)
            def _():
                c = s - lag
                wait_a(kk, c)

                @pl.when(goes_right[kk])
                def _():
                    right(kk, c).start()

                @pl.when(goes_left[kk])
                def _():
                    left(kk, c).start()

        @pl.when(in_range(s, WAY_LAG) & is_way)
        def _():
            c = s - WAY_LAG
            for i2 in range(2):
                wait_slot(tr, sem_tr, i2, c)
                up(i2, c).start()
        return 0

    lax.fori_loop(0, CHUNKS + FAR_LAG, relay, 0)

    def b_relays(c):
        wait_slot(pb, sem_b, far_row, c)
        b_relay(c).start()

    for_chunks(b_relays)

    def drain(c):
        for r in (2 * y + 1 - core, 2 * (1 - y) + 1 - core):
            wait_slot(pb, sem_b, r, c)
        for kk in range(4):
            @pl.when(jnp.logical_not(goes[kk]))
            def _():
                wait_a(kk, c)

        @pl.when(jnp.logical_not(own_home))
        def _():
            to_home(c).wait_send()

        @pl.when(jnp.logical_not(home))
        def _():
            to_transit(c).wait_send()
        b_far(c).wait_send()
        b_near(c).wait_send()
        b_relay(c).wait_send()
        for kk in range(4):
            @pl.when(goes_right[kk])
            def _():
                right(kk, c).wait_send()

            @pl.when(goes_left[kk])
            def _():
                left(kk, c).wait_send()

        @pl.when(is_way)
        def _():
            for i2 in range(2):
                up(i2, c).wait_send()

    for_chunks(drain)
    out_b.wait()


def move(a, b):
    tile = (64, 3, 96, 128)
    any_spec = pl.BlockSpec(memory_space=pltpu.HBM)
    pa, pb, _ = pl.pallas_call(
        move_kernel,
        out_shape=[jax.ShapeDtypeStruct((n,) + tile, jnp.bfloat16) for n in (4, 4, 2)],
        in_specs=[any_spec] * 2,
        out_specs=[any_spec] * 3,
        scratch_shapes=[
            pltpu.VMEM(tile, jnp.bfloat16),
            pltpu.VMEM(tile, jnp.bfloat16),
            pltpu.SemaphoreType.DMA((4, CHUNKS)),
            pltpu.SemaphoreType.DMA((4, CHUNKS)),
            pltpu.SemaphoreType.DMA((2, CHUNKS)),
            pltpu.SemaphoreType.DMA((15, CHUNKS)),
            pltpu.SemaphoreType.DMA((4,)),
        ],
        compiler_params=pltpu.CompilerParams(has_side_effects=True),
    )(a, b)
    return pa, pb


H_STEP = 4
E_STEPS = 64 // H_STEP
I_STEP = 16


def finish_kernel(pa_ref, pb_ref, z_ref, gin_ref, gout_ref, wg_ref, wo_ref, out_ref, o_ref):
    step = pl.program_id(0)

    @pl.when(step < E_STEPS)
    def _():
        def one(h, _):
            def sides(ref):
                sec = [ref[:, h, s].reshape(384, 128) for s in range(3)]
                return jnp.concatenate([sec[0], sec[2]], axis=1), jnp.concatenate([sec[1], sec[2]], axis=1)

            a_lo, a_hi = sides(pa_ref)
            b_lo, b_hi = sides(pb_ref)
            dims = (((0,), (0,)), ((), ()))
            lo = lax.dot_general(a_lo, b_lo, dims, preferred_element_type=jnp.float32)
            hi = lax.dot_general(a_hi, b_hi, dims, preferred_element_type=jnp.float32)
            hh = step * H_STEP + h
            o_ref[hh, 0:128, 0:128] = lo[0:128, 0:128] + hi[0:128, 0:128]
            o_ref[hh, 128:192, 0:128] = lo[128:192, 0:128] + hi[192:256, 0:128]
            right = jnp.concatenate(
                [lo[0:128, 128:192] + hi[0:128, 192:256], lo[128:192, 128:192] + lo[192:256, 192:256]], axis=0)
            o_ref[hh, :, 128:192] = right
            return 0

        lax.fori_loop(0, H_STEP, one, 0)

    @pl.when(step >= E_STEPS)
    def _():
        base = (step - E_STEPS) * I_STEP
        for q in range(I_STEP // 8):
            rows = pl.ds(pl.multiple_of(base + 8 * q, 8), 8)
            o = o_ref[:, rows, :]
            yv = norm_channels(o, gout_ref[...], 0).astype(jnp.bfloat16).reshape(512, 192)
            upd = jnp.dot(wo_ref[...], yv, preferred_element_type=jnp.float32)
            zv = z_ref[8 * q:8 * q + 8].astype(jnp.float32)
            x = norm_channels(zv, gin_ref[...][None], 1).astype(jnp.bfloat16).reshape(2, 256, 192)
            for s in range(2):
                gate = sigmoid(jnp.dot(wg_ref[...], x[s], preferred_element_type=jnp.float32))
                res = zv[4 * s:4 * s + 4].reshape(256, 192) + gate * upd[256 * s:256 * s + 256]
                out_ref[8 * q + 4 * s:8 * q + 4 * s + 4] = res.astype(jnp.bfloat16).reshape(4, 64, 192)


def finish(pa, pb, z, gin, gout, wg, wo):
    panel = pl.BlockSpec((4, H_STEP, 3, 96, 128), lambda i: (0, jnp.minimum(i, E_STEPS - 1), 0, 0, 0))
    rows = pl.BlockSpec((I_STEP, 64, 192), lambda i: (jnp.maximum(i - E_STEPS, 0), 0, 0))
    full2 = lambda i: (0, 0)
    return pl.pallas_call(
        finish_kernel,
        grid=(E_STEPS + 192 // I_STEP,),
        out_shape=jax.ShapeDtypeStruct((192, 64, 192), jnp.bfloat16),
        in_specs=[
            panel, panel, rows,
            pl.BlockSpec((64, 1), full2),
            pl.BlockSpec((64, 1, 1), lambda i: (0, 0, 0)),
            pl.BlockSpec((256, 256), full2),
            pl.BlockSpec((512, 512), full2),
        ],
        out_specs=rows,
        scratch_shapes=[pltpu.VMEM((64, 192, 192), jnp.float32)],
        compiler_params=pltpu.CompilerParams(vmem_limit_bytes=48 * 1024 * 1024),
    )(pa, pb, z, gin, gout, wg, wo)


def spread(w, n, swap=False):
    t = w.T
    if swap:
        t = t.reshape(32, 2, 64)[:, ::-1].reshape(64, 64)
    eye = jnp.eye(n, dtype=w.dtype)
    return (t[:, None, None, :] * eye[None, :, :, None]).reshape(64 * n, 64 * n)


def solution(mesh):
    tile_spec = P(('batch', 'row'), 'col', None)
    mask_spec = P(('batch', 'row'), 'col')
    replicated = P()

    def local_step(pair, mask, gin, w_l, w_lg, w_r, w_rg, w_g, gout, w_o):
        z = jnp.transpose(pair, (0, 2, 1))
        gin_c = gin.astype(jnp.float32)[:, None]
        gout_c = gout.astype(jnp.float32)[:, None, None]
        w_even = jnp.concatenate([spread(w, 4) for w in (w_l, w_lg, w_r, w_rg)], axis=0)
        w_odd = jnp.concatenate([spread(w, 4, True) for w in (w_l, w_lg, w_r, w_rg)], axis=0)
        eye4, eye8 = jnp.eye(4, dtype=w_g.dtype), jnp.eye(8, dtype=w_o.dtype)
        wg4 = (eye4[:, None, :, None] * w_g.T[None, :, None, :]).reshape(256, 256)
        wo8 = (eye8[:, None, None, :] * w_o.T[None, :, :, None]).reshape(512, 512)
        a, b = project(z, mask, gin_c, w_even, w_odd)
        pa, pb = move(a, b)
        out = finish(pa, pb, z, gin_c, gout_c, wg4, wo8)
        return jnp.transpose(out, (0, 2, 1))

    return jax.shard_map(local_step, mesh=mesh, in_specs=(tile_spec, mask_spec) + (replicated,) * 8, out_specs=tile_spec, check_vma=False)
```

```python
import jax
import jax.numpy as jnp
from jax import lax
from jax.experimental import pallas as pl
from jax.experimental.pallas import tpu as pltpu
from jax.sharding import PartitionSpec as P

LN_EPS = 0.00001
MESH = pl.DeviceIdType.MESH
CHUNKS = 16
WAY_LAG = 5
FAR_LAG = 10
B_LAG = 9
SUM_LAG = 13


def sigmoid(v):
    return 0.5 * jnp.tanh(0.5 * v) + 0.5


def norm_channels(v, gain, axis):
    mean = jnp.mean(v, axis=axis, keepdims=True)
    cen = v - mean
    var = jnp.mean(cen * cen, axis=axis, keepdims=True)
    return cen * lax.rsqrt(var + LN_EPS) * gain


def project_kernel(z_ref, m_ref, gin_ref, we_ref, wo_ref, a_ref, b_ref):
    gain = gin_ref[...][None]
    for half in range(2):
        z = z_ref[16 * half:16 * half + 16].astype(jnp.float32)
        x = norm_channels(z, gain, 1).astype(jnp.bfloat16).reshape(4, 256, 192)
        m = m_ref[16 * half:16 * half + 16].astype(jnp.float32)

        def lanes(p, q):
            return jnp.concatenate([p[:, :128], q[:, :128], p[:, 128:], q[:, 128:]], axis=1)

        acts = []
        for par, w_ref in ((0, we_ref), (1, wo_ref)):
            rhs = lanes(x[par], x[par + 2])
            keep = lanes(m[4 * par:4 * par + 4], m[4 * par + 8:4 * par + 12])
            keep = jnp.concatenate([keep, keep], axis=0)[None]
            proj = jnp.dot(w_ref[...], rhs, preferred_element_type=jnp.float32)
            proj = proj.reshape(4, 32, 8, 384)
            acts.append((keep * sigmoid(proj[1]) * proj[0], keep * sigmoid(proj[3]) * proj[2]))
        low = lax.broadcasted_iota(jnp.int32, (32, 8, 384), 1) < 4
        for e, o, ref in ((acts[0][0], acts[1][0], a_ref), (acts[0][1], acts[1][1], b_ref)):
            first = jnp.where(low, e, o)
            second = jnp.where(low, o, e)
            both = jnp.stack([first, second], axis=1).reshape(64, 8, 384).astype(jnp.bfloat16)
            for sec in range(3):
                ref[:, sec, 8 * half:8 * half + 8, :] = both[:, :, 128 * sec:128 * sec + 128]


def project(z, m, gin, w_even, w_odd):
    full = lambda i: (0, 0)
    tile = jax.ShapeDtypeStruct((64, 3, 96, 128), jnp.bfloat16)
    out_spec = pl.BlockSpec((64, 3, 16, 128), lambda i: (0, 0, i, 0))
    return pl.pallas_call(
        project_kernel,
        grid=(6,),
        out_shape=[tile, tile],
        in_specs=[
            pl.BlockSpec((32, 64, 192), lambda i: (i, 0, 0)),
            pl.BlockSpec((32, 192), lambda i: (i, 0)),
            pl.BlockSpec((64, 1), full),
            pl.BlockSpec((1024, 256), full),
            pl.BlockSpec((1024, 256), full),
        ],
        out_specs=[out_spec, out_spec],
        compiler_params=pltpu.CompilerParams(vmem_limit_bytes=60 * 1024 * 1024),
    )(z, m, gin, w_even, w_odd)


def channel_sum(pa, pb, h, buf, at):
    def sides(ref):
        sec = [ref[:, h, s].reshape(384, 128) for s in range(3)]
        return jnp.concatenate([sec[0], sec[2]], axis=1), jnp.concatenate([sec[1], sec[2]], axis=1)

    a_lo, a_hi = sides(pa)
    b_lo, b_hi = sides(pb)
    dims = (((0,), (0,)), ((), ()))
    lo = lax.dot_general(a_lo, b_lo, dims, preferred_element_type=jnp.float32)
    hi = lax.dot_general(a_hi, b_hi, dims, preferred_element_type=jnp.float32)
    buf[at + (slice(0, 128), slice(0, 128))] = lo[0:128, 0:128] + hi[0:128, 0:128]
    buf[at + (slice(128, 192), slice(0, 128))] = lo[128:192, 0:128] + hi[192:256, 0:128]
    buf[at + (slice(None), slice(128, 192))] = jnp.concatenate(
        [lo[0:128, 128:192] + hi[0:128, 192:256], lo[128:192, 128:192] + lo[192:256, 192:256]], axis=0)


def move_kernel(a_ref, b_ref, o_ref, tr, pa, pb, buf, sem_a, sem_b, sem_tr, snd, loc, out_sem):
    bat, z, row = lax.axis_index('batch'), lax.axis_index('col'), lax.axis_index('row')
    y, core = row // 2, row % 2
    size = 64 // CHUNKS

    def flip(v, n, fam):
        return jnp.where(fam == 0, v, n - v)

    def dev(col, r):
        return {'batch': bat, 'col': col, 'row': r}

    def rc(src, dst, send, recv, col, r):
        return pltpu.make_async_remote_copy(
            src_ref=src, dst_ref=dst, send_sem=send, recv_sem=recv, device_id=dev(col, r), device_id_type=MESH)

    def part(ref, c):
        return ref.at[pl.ds(c * size, size)]

    def slot(ref, s, c):
        return ref.at[s, pl.ds(c * size, size)]

    fam = z // 2
    blk = flip(z, 3, fam)
    home = y == fam
    k_src = flip(row, 3, fam)

    def to_home(c):
        return rc(part(a_ref, c), slot(pa, row, c), snd.at[0, c], sem_a.at[row, c], z, z)

    def to_transit(c):
        return rc(part(a_ref, c), slot(tr, blk, c), snd.at[1, c], sem_tr.at[blk, c], flip(k_src, 3, fam), flip(5 - k_src, 3, fam))

    def b_far(c):
        return rc(part(b_ref, c), slot(pb, row, c), snd.at[2, c], sem_b.at[row, c], z, 2 * (1 - y) + core)

    def b_near(c):
        return rc(part(b_ref, c), slot(pb, row, c), snd.at[3, c], sem_b.at[row, c], z, 2 * y + 1 - core)

    far_row = 2 * (1 - y) + core

    def b_relay(c):
        return rc(slot(pb, far_row, c), slot(pb, far_row, c), snd.at[4, c], sem_b.at[far_row, c], z, 2 * y + 1 - core)

    zz, ii = flip(z, 3, y), flip(row, 3, y)

    def real(kk):
        return flip(jnp.int32(kk), 3, y)

    def right(kk, c):
        k = real(kk)
        return rc(slot(pa, k, c), slot(pa, k, c), snd.at[5 + kk, c], sem_a.at[k, c], jnp.where(y == 0, z + 1, z - 1), row)

    def left(kk, c):
        k = real(kk)
        return rc(slot(pa, k, c), slot(pa, k, c), snd.at[9 + kk, c], sem_a.at[k, c], jnp.where(y == 0, z - 1, z + 1), row)

    ofam = 1 - y
    oz, ok = flip(z, 3, ofam), flip(row, 3, ofam)
    is_way = (oz >= 2) & (ok == 5 - oz)
    way_k = flip(oz, 3, ofam)

    def up(i2, c):
        return rc(slot(tr, i2, c), slot(pa, way_k, c), snd.at[13 + i2, c], sem_a.at[way_k, c], z, flip(jnp.int32(i2), 3, ofam))

    is_src = (ii == zz)
    own_home = home & (row == z)

    cp_a = pltpu.make_async_copy(a_ref, pa.at[row], loc.at[0])
    cp_b = pltpu.make_async_copy(b_ref, pb.at[row], loc.at[1])

    @pl.when(own_home)
    def _():
        cp_a.start()

    cp_b.start()

    def for_chunks(f):
        def body(c, _):
            f(c)
            return 0
        lax.fori_loop(0, CHUNKS, body, 0)

    def first_sends(c):
        @pl.when(jnp.logical_not(own_home))
        def _():
            to_home(c).start()

        @pl.when(jnp.logical_not(home))
        def _():
            to_transit(c).start()

    for_chunks(first_sends)

    @pl.when(own_home)
    def _():
        cp_a.wait()

    cp_b.wait()

    def wait_a(kk, c):
        k = real(kk)

        @pl.when(jnp.logical_not(own_home & (k == row)))
        def _():
            rc(slot(pa, k, c), slot(pa, k, c), snd.at[0, c], sem_a.at[k, c], z, row).wait_recv()

    goes_right = [
        ((zz == 0) & is_src) | ((zz == 1)) | (zz == 2),
        ((zz == 0) & is_src) | ((zz == 1)) | (zz == 2),
        ((zz == 0) & is_src) | (zz == 2),
        ((zz == 0) & is_src),
    ]
    goes_left = [
        (zz == 1) & is_src,
        (zz == 1) & is_src,
        (zz == 1) & is_src,
        ((zz == 1) & is_src) | (zz == 3),
    ]

    def wait_slot(ref, sem, s, c):
        rc(slot(ref, s, c), slot(ref, s, c), snd.at[0, c], sem.at[s, c], z, row).wait_recv()

    goes = [goes_right[kk] | goes_left[kk] for kk in range(4)]
    near_lag = [0, 0, 1, 1]
    forwards = []
    for kk in range(4):
        forwards.append((near_lag[kk], kk, goes[kk] & (zz < 2) & is_src))
    for kk in range(2):
        forwards.append((1, kk, (zz == 1) & jnp.logical_not(is_src)))
        forwards.append((2, kk, zz == 2))
    forwards.append((FAR_LAG, 2, zz == 2))
    forwards.append((FAR_LAG, 3, zz == 3))
    forwards.sort(key=lambda f: f[0])

    def in_range(s, lag):
        return (s >= lag) & (s < CHUNKS + lag)

    def relay(s, _):
        @pl.when(s < CHUNKS)
        def _():
            b_far(s).start()
            b_near(s).start()

        for lag, kk, who in forwards:
            @pl.when(in_range(s, lag) & who)
            def _():
                c = s - lag
                wait_a(kk, c)

                @pl.when(goes_right[kk])
                def _():
                    right(kk, c).start()

                @pl.when(goes_left[kk])
                def _():
                    left(kk, c).start()

        @pl.when(in_range(s, WAY_LAG) & is_way)
        def _():
            c = s - WAY_LAG
            for i2 in range(2):
                wait_slot(tr, sem_tr, i2, c)
                up(i2, c).start()
        @pl.when(in_range(s, B_LAG))
        def _():
            c = s - B_LAG
            wait_slot(pb, sem_b, far_row, c)
            b_relay(c).start()

        @pl.when(in_range(s, SUM_LAG))
        def _():
            c = s - SUM_LAG
            for r in (2 * y + 1 - core, 2 * (1 - y) + 1 - core):
                wait_slot(pb, sem_b, r, c)
            for kk in range(4):
                @pl.when(jnp.logical_not(goes[kk]))
                def _():
                    wait_a(kk, c)

            @pl.when(c >= 2)
            def _():
                sum_out(c - 2).wait()

            def one(h, _):
                channel_sum(pa, pb, c * size + h, buf, (c % 2, h))
                return 0

            lax.fori_loop(0, size, one, 0)
            sum_out(c).start()
        return 0

    def sum_out(c):
        return pltpu.make_async_copy(buf.at[c % 2], part(o_ref, c), out_sem.at[c % 2])

    lax.fori_loop(0, CHUNKS + SUM_LAG, relay, 0)
    for c in range(CHUNKS - 2, CHUNKS):
        sum_out(c).wait()

    def drain(c):
        @pl.when(jnp.logical_not(own_home))
        def _():
            to_home(c).wait_send()

        @pl.when(jnp.logical_not(home))
        def _():
            to_transit(c).wait_send()
        b_far(c).wait_send()
        b_near(c).wait_send()
        b_relay(c).wait_send()
        for kk in range(4):
            @pl.when(goes_right[kk])
            def _():
                right(kk, c).wait_send()

            @pl.when(goes_left[kk])
            def _():
                left(kk, c).wait_send()

        @pl.when(is_way)
        def _():
            for i2 in range(2):
                up(i2, c).wait_send()

    for_chunks(drain)


def move(a, b):
    tile = (64, 3, 96, 128)
    any_spec = pl.BlockSpec(memory_space=pltpu.HBM)
    o, _ = pl.pallas_call(
        move_kernel,
        out_shape=[jax.ShapeDtypeStruct((64, 192, 192), jnp.float32), jax.ShapeDtypeStruct((2,) + tile, jnp.bfloat16)],
        in_specs=[any_spec] * 2,
        out_specs=[any_spec] * 2,
        scratch_shapes=[
            pltpu.VMEM((4,) + tile, jnp.bfloat16),
            pltpu.VMEM((4,) + tile, jnp.bfloat16),
            pltpu.VMEM((2, 64 // CHUNKS, 192, 192), jnp.float32),
            pltpu.SemaphoreType.DMA((4, CHUNKS)),
            pltpu.SemaphoreType.DMA((4, CHUNKS)),
            pltpu.SemaphoreType.DMA((2, CHUNKS)),
            pltpu.SemaphoreType.DMA((15, CHUNKS)),
            pltpu.SemaphoreType.DMA((2,)),
            pltpu.SemaphoreType.DMA((2,)),
        ],
        compiler_params=pltpu.CompilerParams(has_side_effects=True, vmem_limit_bytes=60 * 1024 * 1024),
    )(a, b)
    return o


I_STEP = 16


def finish_kernel(o_ref, z_ref, gin_ref, gout_ref, wg_ref, wo_ref, out_ref):
    for q in range(I_STEP // 8):
        o = o_ref[:, 8 * q:8 * q + 8, :]
        yv = norm_channels(o, gout_ref[...], 0).astype(jnp.bfloat16).reshape(512, 192)
        upd = jnp.dot(wo_ref[...], yv, preferred_element_type=jnp.float32)
        zv = z_ref[8 * q:8 * q + 8].astype(jnp.float32)
        x = norm_channels(zv, gin_ref[...][None], 1).astype(jnp.bfloat16).reshape(2, 256, 192)
        for s in range(2):
            gate = sigmoid(jnp.dot(wg_ref[...], x[s], preferred_element_type=jnp.float32))
            res = zv[4 * s:4 * s + 4].reshape(256, 192) + gate * upd[256 * s:256 * s + 256]
            out_ref[8 * q + 4 * s:8 * q + 4 * s + 4] = res.astype(jnp.bfloat16).reshape(4, 64, 192)


def finish(o, z, gin, gout, wg, wo):
    rows = pl.BlockSpec((I_STEP, 64, 192), lambda i: (i, 0, 0))
    full2 = lambda i: (0, 0)
    return pl.pallas_call(
        finish_kernel,
        grid=(192 // I_STEP,),
        out_shape=jax.ShapeDtypeStruct((192, 64, 192), jnp.bfloat16),
        in_specs=[
            pl.BlockSpec((64, I_STEP, 192), lambda i: (0, i, 0)), rows,
            pl.BlockSpec((64, 1), full2),
            pl.BlockSpec((64, 1, 1), lambda i: (0, 0, 0)),
            pl.BlockSpec((256, 256), full2),
            pl.BlockSpec((512, 512), full2),
        ],
        out_specs=rows,
        compiler_params=pltpu.CompilerParams(vmem_limit_bytes=60 * 1024 * 1024),
    )(o, z, gin, gout, wg, wo)


def spread(w, n, swap=False):
    t = w.T
    if swap:
        t = t.reshape(32, 2, 64)[:, ::-1].reshape(64, 64)
    eye = jnp.eye(n, dtype=w.dtype)
    return (t[:, None, None, :] * eye[None, :, :, None]).reshape(64 * n, 64 * n)


def solution(mesh):
    tile_spec = P(('batch', 'row'), 'col', None)
    mask_spec = P(('batch', 'row'), 'col')
    replicated = P()

    def local_step(pair, mask, gin, w_l, w_lg, w_r, w_rg, w_g, gout, w_o):
        z = jnp.transpose(pair, (0, 2, 1))
        gin_c = gin.astype(jnp.float32)[:, None]
        gout_c = gout.astype(jnp.float32)[:, None, None]
        w_even = jnp.concatenate([spread(w, 4) for w in (w_l, w_lg, w_r, w_rg)], axis=0)
        w_odd = jnp.concatenate([spread(w, 4, True) for w in (w_l, w_lg, w_r, w_rg)], axis=0)
        eye4, eye8 = jnp.eye(4, dtype=w_g.dtype), jnp.eye(8, dtype=w_o.dtype)
        wg4 = (eye4[:, None, :, None] * w_g.T[None, :, None, :]).reshape(256, 256)
        wo8 = (eye8[:, None, None, :] * w_o.T[None, :, :, None]).reshape(512, 512)
        a, b = project(z, mask, gin_c, w_even, w_odd)
        o = move(a, b)
        out = finish(o, z, gin_c, gout_c, wg4, wo8)
        return jnp.transpose(out, (0, 2, 1))

    return jax.shard_map(local_step, mesh=mesh, in_specs=(tile_spec, mask_spec) + (replicated,) * 8, out_specs=tile_spec, check_vma=False)
```

```python
import jax
import jax.numpy as jnp
from jax import lax
from jax.experimental import pallas as pl
from jax.experimental.pallas import tpu as pltpu
from jax.sharding import PartitionSpec as P

LN_EPS = 0.00001
MESH = pl.DeviceIdType.MESH
CHUNKS = 32
NEAR_LAG = 1
CROSS_LAG = 2
HOP_LAG = 3
PASS_LAG = 5
WAY_LAG = 3
B_LAG = 3
EDGE_LAG = 3
SHARE_LAG = 6
SUM_LAG = 9


def sigmoid(v):
    return 0.5 * jnp.tanh(0.5 * v) + 0.5


def norm_channels(v, gain, axis):
    mean = jnp.mean(v, axis=axis, keepdims=True)
    cen = v - mean
    var = jnp.mean(cen * cen, axis=axis, keepdims=True)
    return cen * lax.rsqrt(var + LN_EPS) * gain


def project_kernel(z_ref, m_ref, gin_ref, we_ref, wo_ref, a_ref, b_ref):
    gain = gin_ref[...][None]
    for half in range(2):
        z = z_ref[16 * half:16 * half + 16].astype(jnp.float32)
        x = norm_channels(z, gain, 1).astype(jnp.bfloat16).reshape(4, 256, 192)
        m = m_ref[16 * half:16 * half + 16].astype(jnp.float32)

        def lanes(p, q):
            return jnp.concatenate([p[:, :128], q[:, :128], p[:, 128:], q[:, 128:]], axis=1)

        acts = []
        for par, w_ref in ((0, we_ref), (1, wo_ref)):
            rhs = lanes(x[par], x[par + 2])
            keep = lanes(m[4 * par:4 * par + 4], m[4 * par + 8:4 * par + 12])
            keep = jnp.concatenate([keep, keep], axis=0)[None]
            proj = jnp.dot(w_ref[...], rhs, preferred_element_type=jnp.float32)
            proj = proj.reshape(4, 32, 8, 384)
            acts.append((keep * sigmoid(proj[1]) * proj[0], keep * sigmoid(proj[3]) * proj[2]))
        low = lax.broadcasted_iota(jnp.int32, (32, 8, 384), 1) < 4
        for e, o, ref in ((acts[0][0], acts[1][0], a_ref), (acts[0][1], acts[1][1], b_ref)):
            first = jnp.where(low, e, o)
            second = jnp.where(low, o, e)
            both = jnp.stack([first, second], axis=1).reshape(64, 8, 384).astype(jnp.bfloat16)
            for sec in range(3):
                ref[:, sec, 8 * half:8 * half + 8, :] = both[:, :, 128 * sec:128 * sec + 128]


def project(z, m, gin, w_even, w_odd):
    full = lambda i: (0, 0)
    tile = jax.ShapeDtypeStruct((64, 3, 96, 128), jnp.bfloat16)
    out_spec = pl.BlockSpec((64, 3, 16, 128), lambda i: (0, 0, i, 0))
    return pl.pallas_call(
        project_kernel,
        grid=(6,),
        out_shape=[tile, tile],
        in_specs=[
            pl.BlockSpec((32, 64, 192), lambda i: (i, 0, 0)),
            pl.BlockSpec((32, 192), lambda i: (i, 0)),
            pl.BlockSpec((64, 1), full),
            pl.BlockSpec((1024, 256), full),
            pl.BlockSpec((1024, 256), full),
        ],
        out_specs=[out_spec, out_spec],
        compiler_params=pltpu.CompilerParams(vmem_limit_bytes=60 * 1024 * 1024),
    )(z, m, gin, w_even, w_odd)


def channel_sum(pa, pb, h, buf, at):
    def sides(ref):
        sec = [ref[:, h, s].reshape(384, 128) for s in range(3)]
        return jnp.concatenate([sec[0], sec[2]], axis=1), jnp.concatenate([sec[1], sec[2]], axis=1)

    a_lo, a_hi = sides(pa)
    b_lo, b_hi = sides(pb)
    dims = (((0,), (0,)), ((), ()))
    lo = lax.dot_general(a_lo, b_lo, dims, preferred_element_type=jnp.float32)
    hi = lax.dot_general(a_hi, b_hi, dims, preferred_element_type=jnp.float32)
    wide = jnp.concatenate([lo[0:128, 0:128] + hi[0:128, 0:128], lo[128:192, 0:128] + hi[192:256, 0:128]], axis=0)
    rest = jnp.concatenate(
        [lo[0:128, 128:192] + hi[0:128, 192:256], lo[128:192, 128:192] + lo[192:256, 192:256]], axis=0)
    buf[at + (0,)] = wide[0:96]
    buf[at + (1,)] = wide[96:192]
    buf[at + (2,)] = jnp.concatenate([rest[0:96], rest[96:192]], axis=1)


def move_kernel(a_ref, b_ref, o_ref, tr, pa, pb, pe, buf, sem_a, sem_b, sem_e, sem_tr, sem_o, snd, loc, out_sem):
    bat, z, row = lax.axis_index('batch'), lax.axis_index('col'), lax.axis_index('row')
    y, core = row // 2, row % 2
    size = 64 // CHUNKS

    def flip(v, n, fam):
        return jnp.where(fam == 0, v, n - v)

    def dev(col, r):
        return {'batch': bat, 'col': col, 'row': r}

    def rc(src, dst, send, recv, col, r):
        return pltpu.make_async_remote_copy(
            src_ref=src, dst_ref=dst, send_sem=send, recv_sem=recv, device_id=dev(col, r), device_id_type=MESH)

    def part(ref, c):
        return ref.at[pl.ds(c * size, size)]

    def slot(ref, s, c):
        return ref.at[s, pl.ds(c * size, size)]

    def wait_slot(ref, sem, s, c):
        rc(slot(ref, s, c), slot(ref, s, c), snd.at[0, c], sem.at[s, c], z, row).wait_recv()

    partner, across = 2 * y + 1 - core, 2 * (1 - y) + core
    diagonal = 2 * (1 - y) + 1 - core

    fam = z // 2
    blk = flip(z, 3, fam)
    home = y == fam
    k_src = flip(row, 3, fam)
    own_home = home & (row == z)
    sends_far = jnp.logical_not(home) & ((k_src == 3) | (blk == 1))

    def to_home(c):
        return rc(part(a_ref, c), slot(pa, row, c), snd.at[0, c], sem_a.at[row, c], z, z)

    def to_way(c):
        return rc(part(a_ref, c), slot(tr, blk, c), snd.at[1, c], sem_tr.at[blk, c], flip(jnp.int32(2), 3, fam), row)

    zz, ii = flip(z, 3, y), flip(row, 3, y)
    is_src = ii == zz
    inner = jnp.where(y == 0, z - 1, z + 1)
    outer = jnp.where(y == 0, z + 1, z - 1)

    def real(kk):
        return flip(jnp.int32(kk), 3, y)

    def hop(kk, c, n, col):
        k = real(kk)
        return rc(slot(pa, k, c), slot(pa, k, c), snd.at[n + kk, c], sem_a.at[k, c], col, row)

    def right(kk, c):
        return hop(kk, c, 2, outer)

    def left(kk, c):
        return hop(kk, c, 6, inner)

    goes_right = [
        (zz == 1) | ((zz == 0) & is_src),
        (zz == 1) | ((zz == 0) & is_src),
        ((zz == 1) & (ii == 0)) | ((zz == 0) & is_src),
        (zz == 0) & is_src,
    ]
    goes_left = [(zz == 1) & is_src] * 4
    goes = [goes_right[kk] | goes_left[kk] for kk in range(4)]

    ofam = 1 - y
    oz, ok = flip(z, 3, ofam), flip(row, 3, ofam)
    ways = [(oz == 2) & (ok == 3), oz == 2]

    def up(i2, c):
        return rc(slot(tr, i2, c), slot(pa, row, c), snd.at[10 + i2, c], sem_a.at[row, c], z, flip(jnp.int32(i2), 3, ofam))

    is_edge, is_inner = zz == 3, zz == 2
    not_edge = jnp.logical_not(is_edge)

    def b_far(c):
        return rc(part(b_ref, c), slot(pb, row, c), snd.at[12, c], sem_b.at[row, c], z, across)

    def b_near(c):
        return rc(part(b_ref, c), slot(pb, row, c), snd.at[13, c], sem_b.at[row, c], z, partner)

    def b_relay(c):
        return rc(slot(pb, across, c), slot(pb, across, c), snd.at[14, c], sem_b.at[across, c], z, partner)

    def e_own(c):
        return rc(part(b_ref, c), slot(pe, row, c), snd.at[13, c], sem_e.at[row, c], inner, row)

    def e_far(c):
        return rc(slot(pb, across, c), slot(pe, across, c), snd.at[14, c], sem_e.at[across, c], inner, row)

    def e_share(r, n, c):
        return rc(slot(pe, r, c), slot(pe, r, c), snd.at[n, c], sem_e.at[r, c], z, partner)

    def o_edge(c):
        return rc(buf.at[2 + c % 2], part(o_ref, c), snd.at[17, c], sem_o.at[c], outer, row)

    def o_own(c):
        return pltpu.make_async_copy(buf.at[c % 2], part(o_ref, c), out_sem.at[c % 2])

    def for_chunks(f):
        def body(c, _):
            f(c)
            return 0
        lax.fori_loop(0, CHUNKS, body, 0)

    cp_a = pltpu.make_async_copy(a_ref, pa.at[row], loc.at[0])
    cp_b = pltpu.make_async_copy(b_ref, pb.at[row], loc.at[1])

    @pl.when(own_home)
    def _():
        cp_a.start()

    cp_b.start()

    @pl.when(own_home)
    def _():
        cp_a.wait()

    cp_b.wait()

    def wait_a(kk, c):
        k = real(kk)

        @pl.when(jnp.logical_not(own_home & (k == row)))
        def _():
            wait_slot(pa, sem_a, k, c)

    forwards = [(NEAR_LAG, 0, (zz < 2) & is_src), (NEAR_LAG, 1, (zz < 2) & is_src)]
    forwards += [(CROSS_LAG, kk, (zz < 2) & is_src) for kk in (2, 3)]
    forwards += [(HOP_LAG, kk, (zz == 1) & (ii == 0)) for kk in (0, 1)]
    forwards += [(PASS_LAG, 2, (zz == 1) & (ii == 0))]

    def in_range(s, lag):
        return (s >= lag) & (s < CHUNKS + lag)

    def step(s, _):
        @pl.when(s < CHUNKS)
        def _():
            @pl.when(jnp.logical_not(own_home))
            def _():
                to_home(s).start()

            @pl.when(sends_far)
            def _():
                to_way(s).start()

            b_far(s).start()

            @pl.when(is_edge)
            def _():
                e_own(s).start()

            @pl.when(not_edge)
            def _():
                b_near(s).start()

        for lag, kk, who in forwards:
            @pl.when(in_range(s, lag) & who)
            def _():
                c = s - lag
                wait_a(kk, c)

                @pl.when(goes_right[kk])
                def _():
                    right(kk, c).start()

                @pl.when(goes_left[kk])
                def _():
                    left(kk, c).start()

        @pl.when(in_range(s, WAY_LAG))
        def _():
            c = s - WAY_LAG
            for i2 in range(2):
                @pl.when(ways[i2])
                def _():
                    wait_slot(tr, sem_tr, i2, c)
                    up(i2, c).start()

        @pl.when(in_range(s, EDGE_LAG) & is_edge)
        def _():
            c = s - EDGE_LAG
            wait_slot(pb, sem_b, across, c)
            e_far(c).start()

        @pl.when(in_range(s, B_LAG) & not_edge)
        def _():
            c = s - B_LAG
            wait_slot(pb, sem_b, across, c)
            b_relay(c).start()

        for lag, r, n in ((EDGE_LAG, row, 15), (SHARE_LAG, across, 16)):
            @pl.when(in_range(s, lag) & is_inner)
            def _():
                c = s - lag
                wait_slot(pe, sem_e, r, c)
                e_share(r, n, c).start()

        @pl.when(in_range(s, SUM_LAG) & not_edge)
        def _():
            c = s - SUM_LAG
            for r in (partner, diagonal):
                wait_slot(pb, sem_b, r, c)
            for kk in range(4):
                @pl.when(jnp.logical_not(goes[kk]))
                def _():
                    wait_a(kk, c)

            @pl.when(is_inner)
            def _():
                for r in (partner, diagonal):
                    wait_slot(pe, sem_e, r, c)

                @pl.when(c >= 2)
                def _():
                    o_edge(c - 2).wait_send()

                def edge(h, _):
                    channel_sum(pa, pe, c * size + h, buf, (2 + c % 2, h))
                    return 0

                lax.fori_loop(0, size, edge, 0)
                o_edge(c).start()

            @pl.when(c >= 2)
            def _():
                o_own(c - 2).wait()

            def own(h, _):
                channel_sum(pa, pb, c * size + h, buf, (c % 2, h))
                return 0

            lax.fori_loop(0, size, own, 0)
            o_own(c).start()
        return 0

    lax.fori_loop(0, CHUNKS + SUM_LAG, step, 0)

    @pl.when(not_edge)
    def _():
        for c in range(CHUNKS - 2, CHUNKS):
            o_own(c).wait()

    @pl.when(is_inner)
    def _():
        for c in range(CHUNKS - 2, CHUNKS):
            o_edge(c).wait_send()

    def drain(c):
        @pl.when(jnp.logical_not(own_home))
        def _():
            to_home(c).wait_send()

        @pl.when(sends_far)
        def _():
            to_way(c).wait_send()

        b_far(c).wait_send()

        @pl.when(not_edge)
        def _():
            b_near(c).wait_send()
            b_relay(c).wait_send()

        @pl.when(is_edge)
        def _():
            e_own(c).wait_send()
            e_far(c).wait_send()
            rc(buf.at[0], part(o_ref, c), snd.at[0, c], sem_o.at[c], z, row).wait_recv()

        @pl.when(is_inner)
        def _():
            e_share(row, 15, c).wait_send()
            e_share(across, 16, c).wait_send()

        for kk in range(4):
            @pl.when(goes_right[kk])
            def _():
                right(kk, c).wait_send()

            @pl.when(goes_left[kk])
            def _():
                left(kk, c).wait_send()

        for i2 in range(2):
            @pl.when(ways[i2])
            def _():
                up(i2, c).wait_send()

    for_chunks(drain)


def move(a, b):
    tile = (64, 3, 96, 128)
    any_spec = pl.BlockSpec(memory_space=pltpu.HBM)
    o, _ = pl.pallas_call(
        move_kernel,
        out_shape=[jax.ShapeDtypeStruct(tile, jnp.float32), jax.ShapeDtypeStruct((2,) + tile, jnp.bfloat16)],
        in_specs=[any_spec] * 2,
        out_specs=[any_spec] * 2,
        scratch_shapes=[pltpu.VMEM((4,) + tile, jnp.bfloat16)] * 3 + [
            pltpu.VMEM((4, 64 // CHUNKS, 3, 96, 128), jnp.float32),
            pltpu.SemaphoreType.DMA((4, CHUNKS)),
            pltpu.SemaphoreType.DMA((4, CHUNKS)),
            pltpu.SemaphoreType.DMA((4, CHUNKS)),
            pltpu.SemaphoreType.DMA((2, CHUNKS)),
            pltpu.SemaphoreType.DMA((CHUNKS,)),
            pltpu.SemaphoreType.DMA((18, CHUNKS)),
            pltpu.SemaphoreType.DMA((2,)),
            pltpu.SemaphoreType.DMA((2,)),
        ],
        compiler_params=pltpu.CompilerParams(has_side_effects=True, vmem_limit_bytes=67043328),
    )(a, b)
    return o


I_STEP = 16


def finish_kernel(wide_ref, rest_ref, z_ref, gin_ref, gout_ref, wg_ref, wo_ref, out_ref):
    upper = pl.program_id(0) >= 96 // I_STEP
    for q in range(I_STEP // 8):
        rest = rest_ref[:, 0, 8 * q:8 * q + 8, :]
        rest = jnp.where(upper, rest[:, :, 64:], rest[:, :, :64])
        o = jnp.concatenate([wide_ref[:, 0, 8 * q:8 * q + 8, :], rest], axis=2)
        yv = norm_channels(o, gout_ref[...], 0).astype(jnp.bfloat16).reshape(512, 192)
        upd = jnp.dot(wo_ref[...], yv, preferred_element_type=jnp.float32)
        zv = z_ref[8 * q:8 * q + 8].astype(jnp.float32)
        x = norm_channels(zv, gin_ref[...][None], 1).astype(jnp.bfloat16).reshape(2, 256, 192)
        for s in range(2):
            gate = sigmoid(jnp.dot(wg_ref[...], x[s], preferred_element_type=jnp.float32))
            res = zv[4 * s:4 * s + 4].reshape(256, 192) + gate * upd[256 * s:256 * s + 256]
            out_ref[8 * q + 4 * s:8 * q + 4 * s + 4] = res.astype(jnp.bfloat16).reshape(4, 64, 192)


def finish(o, z, gin, gout, wg, wo):
    rows = pl.BlockSpec((I_STEP, 64, 192), lambda i: (i, 0, 0))
    full2 = lambda i: (0, 0)
    half = 96 // I_STEP
    return pl.pallas_call(
        finish_kernel,
        grid=(192 // I_STEP,),
        out_shape=jax.ShapeDtypeStruct((192, 64, 192), jnp.bfloat16),
        in_specs=[
            pl.BlockSpec((64, 1, I_STEP, 128), lambda i: (0, i // half, i % half, 0)),
            pl.BlockSpec((64, 1, I_STEP, 128), lambda i: (0, 2, i % half, 0)),
            rows,
            pl.BlockSpec((64, 1), full2),
            pl.BlockSpec((64, 1, 1), lambda i: (0, 0, 0)),
            pl.BlockSpec((256, 256), full2),
            pl.BlockSpec((512, 512), full2),
        ],
        out_specs=rows,
        compiler_params=pltpu.CompilerParams(vmem_limit_bytes=60 * 1024 * 1024),
    )(o, o, z, gin, gout, wg, wo)


def spread(w, n, swap=False):
    t = w.T
    if swap:
        t = t.reshape(32, 2, 64)[:, ::-1].reshape(64, 64)
    eye = jnp.eye(n, dtype=w.dtype)
    return (t[:, None, None, :] * eye[None, :, :, None]).reshape(64 * n, 64 * n)


def solution(mesh):
    tile_spec = P(('batch', 'row'), 'col', None)
    mask_spec = P(('batch', 'row'), 'col')
    replicated = P()

    def local_step(pair, mask, gin, w_l, w_lg, w_r, w_rg, w_g, gout, w_o):
        z = jnp.transpose(pair, (0, 2, 1))
        gin_c = gin.astype(jnp.float32)[:, None]
        gout_c = gout.astype(jnp.float32)[:, None, None]
        w_even = jnp.concatenate([spread(w, 4) for w in (w_l, w_lg, w_r, w_rg)], axis=0)
        w_odd = jnp.concatenate([spread(w, 4, True) for w in (w_l, w_lg, w_r, w_rg)], axis=0)
        eye4, eye8 = jnp.eye(4, dtype=w_g.dtype), jnp.eye(8, dtype=w_o.dtype)
        wg4 = (eye4[:, None, :, None] * w_g.T[None, :, None, :]).reshape(256, 256)
        wo8 = (eye8[:, None, None, :] * w_o.T[None, :, :, None]).reshape(512, 512)
        a, b = project(z, mask, gin_c, w_even, w_odd)
        o = move(a, b)
        out = finish(o, z, gin_c, gout_c, wg4, wo8)
        return jnp.transpose(out, (0, 2, 1))

    return jax.shard_map(local_step, mesh=mesh, in_specs=(tile_spec, mask_spec) + (replicated,) * 8, out_specs=tile_spec, check_vma=False)
```

```python
import jax
import jax.numpy as jnp
from jax import lax
from jax.experimental import pallas as pl
from jax.experimental.pallas import tpu as pltpu
from jax.sharding import PartitionSpec as P

LN_EPS = 0.00001
MESH = pl.DeviceIdType.MESH
CHUNKS = 32
NEAR_LAG = 1
CROSS_LAG = 2
HOP_LAG = 3
PASS_LAG = 5
WAY_LAG = 3
B_LAG = 3
EDGE_LAG = 3
SUM_LAG = 9
INNER_LAG = 7


def sigmoid(v):
    return 0.5 * jnp.tanh(0.5 * v) + 0.5


def norm_channels(v, gain, axis):
    mean = jnp.mean(v, axis=axis, keepdims=True)
    cen = v - mean
    var = jnp.mean(cen * cen, axis=axis, keepdims=True)
    return cen * lax.rsqrt(var + LN_EPS) * gain


def lanes(p, q):
    return jnp.concatenate([p[..., :128], q[..., :128], p[..., 128:], q[..., 128:]], axis=-1)


def ids(shape, axis):
    return lax.broadcasted_iota(jnp.int32, shape, axis)


def pick(sel, w):
    return lax.dot_general(sel.astype(jnp.bfloat16), w, (((1,), (1,)), ((), ())), preferred_element_type=jnp.float32)


def column(sel, row):
    return jnp.sum(jnp.where(sel, row.astype(jnp.float32), 0.0), axis=1, keepdims=True)


def project_kernel(z_ref, m_ref, gin_ref, wl_ref, wlg_ref, wr_ref, wrg_ref, a_ref, b_ref, gain_ref, we_ref, wo_ref):
    @pl.when(pl.program_id(0) == 0)
    def _():
        gain_ref[...] = jnp.broadcast_to(column(ids((64, 64), 0) == ids((64, 64), 1), gin_ref[...]), (64, 384))
        chan = ids((256, 64), 0) // 4
        diag = ids((256, 256), 0) % 4 == ids((256, 256), 1) // 64
        for dst, sel in ((we_ref, chan == ids((256, 64), 1)), (wo_ref, chan == (ids((256, 64), 1) ^ 1))):
            for n, w_ref in enumerate((wl_ref, wlg_ref, wr_ref, wrg_ref)):
                t = pick(sel, w_ref[...])
                t = jnp.concatenate([t] * 4, axis=1)
                dst[256 * n:256 * n + 256, :] = jnp.where(diag, t, 0.0).astype(jnp.bfloat16)

    gain = gain_ref[...][None]
    low = ids((32, 8, 384), 1) < 4
    for half in range(2):
        acts = []
        for par, w_ref in ((0, we_ref), (1, wo_ref)):
            r = 16 * half + 4 * par
            z = lanes(z_ref[r:r + 4], z_ref[r + 8:r + 12]).astype(jnp.float32)
            rhs = norm_channels(z, gain, 1).astype(jnp.bfloat16).reshape(256, 384)
            keep = lanes(m_ref[r:r + 4].astype(jnp.float32), m_ref[r + 8:r + 12].astype(jnp.float32))
            keep = jnp.concatenate([keep, keep], axis=0)[None]
            proj = jnp.dot(w_ref[...], rhs, preferred_element_type=jnp.float32)
            proj = proj.reshape(4, 32, 8, 384)
            acts.append((keep * sigmoid(proj[1]) * proj[0], keep * sigmoid(proj[3]) * proj[2]))
        for e, o, ref in ((acts[0][0], acts[1][0], a_ref), (acts[0][1], acts[1][1], b_ref)):
            first = jnp.where(low, e, o)
            second = jnp.where(low, o, e)
            both = jnp.stack([first, second], axis=1).reshape(64, 8, 384).astype(jnp.bfloat16)
            for sec in range(3):
                ref[:, sec, 8 * half:8 * half + 8, :] = both[:, :, 128 * sec:128 * sec + 128]


def project(z, m, gin, w_l, w_lg, w_r, w_rg):
    full = lambda i: (0, 0)
    tile = jax.ShapeDtypeStruct((64, 3, 96, 128), jnp.bfloat16)
    out_spec = pl.BlockSpec((64, 3, 16, 128), lambda i: (0, 0, i, 0))
    return pl.pallas_call(
        project_kernel,
        grid=(6,),
        out_shape=[tile, tile],
        in_specs=[
            pl.BlockSpec((32, 64, 192), lambda i: (i, 0, 0)),
            pl.BlockSpec((32, 192), lambda i: (i, 0)),
            pl.BlockSpec((1, 64), full),
        ] + [pl.BlockSpec((64, 64), full)] * 4,
        out_specs=[out_spec, out_spec],
        scratch_shapes=[
            pltpu.VMEM((64, 384), jnp.float32),
            pltpu.VMEM((1024, 256), jnp.bfloat16),
            pltpu.VMEM((1024, 256), jnp.bfloat16),
        ],
        compiler_params=pltpu.CompilerParams(vmem_limit_bytes=60 * 1024 * 1024),
    )(z, m, gin, w_l, w_lg, w_r, w_rg)


def channel_sum(pa, pb, h, buf, at):
    def sides(ref):
        sec = [ref[:, h, s].reshape(384, 128) for s in range(3)]
        return jnp.concatenate([sec[0], sec[2]], axis=1), jnp.concatenate([sec[1], sec[2]], axis=1)

    a_lo, a_hi = sides(pa)
    b_lo, b_hi = sides(pb)
    dims = (((0,), (0,)), ((), ()))
    lo = lax.dot_general(a_lo, b_lo, dims, preferred_element_type=jnp.float32)
    hi = lax.dot_general(a_hi, b_hi, dims, preferred_element_type=jnp.float32)
    wide = jnp.concatenate([lo[0:128, 0:128] + hi[0:128, 0:128], lo[128:192, 0:128] + hi[192:256, 0:128]], axis=0)
    rest = jnp.concatenate(
        [lo[0:128, 128:192] + hi[0:128, 192:256], lo[128:192, 128:192] + lo[192:256, 192:256]], axis=0)
    buf[at + (0,)] = wide[0:96]
    buf[at + (1,)] = wide[96:192]
    buf[at + (2,)] = jnp.concatenate([rest[0:96], rest[96:192]], axis=1)


def move_kernel(a_ref, b_ref, o_ref, tr, pa, pb, pe, buf, sem_a, sem_b, sem_e, sem_tr, sem_o, snd, loc, out_sem):
    bat, z, row = lax.axis_index('batch'), lax.axis_index('col'), lax.axis_index('row')
    y, core = row // 2, row % 2
    size = 64 // CHUNKS

    def flip(v, n, fam):
        return jnp.where(fam == 0, v, n - v)

    def dev(col, r):
        return {'batch': bat, 'col': col, 'row': r}

    def rc(src, dst, send, recv, col, r):
        return pltpu.make_async_remote_copy(
            src_ref=src, dst_ref=dst, send_sem=send, recv_sem=recv, device_id=dev(col, r), device_id_type=MESH)

    def part(ref, c):
        return ref.at[pl.ds(c * size, size)]

    def slot(ref, s, c):
        return ref.at[s, pl.ds(c * size, size)]

    def wait_slot(ref, sem, s, c):
        rc(slot(ref, s, c), slot(ref, s, c), snd.at[0, c], sem.at[s, c], z, row).wait_recv()

    partner, across = 2 * y + 1 - core, 2 * (1 - y) + core
    diagonal = 2 * (1 - y) + 1 - core

    fam = z // 2
    blk = flip(z, 3, fam)
    home = y == fam
    k_src = flip(row, 3, fam)
    own_home = home & (row == z)
    sends_far = jnp.logical_not(home) & ((k_src == 3) | (blk == 1))

    def to_home(c):
        return rc(part(a_ref, c), slot(pa, row, c), snd.at[0, c], sem_a.at[row, c], z, z)

    def to_way(c):
        return rc(part(a_ref, c), slot(tr, blk, c), snd.at[1, c], sem_tr.at[blk, c], flip(jnp.int32(2), 3, fam), row)

    zz, ii = flip(z, 3, y), flip(row, 3, y)
    is_src = ii == zz
    inner = jnp.where(y == 0, z - 1, z + 1)
    outer = jnp.where(y == 0, z + 1, z - 1)

    def real(kk):
        return flip(jnp.int32(kk), 3, y)

    def hop(kk, c, n, col):
        k = real(kk)
        return rc(slot(pa, k, c), slot(pa, k, c), snd.at[n + kk, c], sem_a.at[k, c], col, row)

    def right(kk, c):
        return hop(kk, c, 2, outer)

    def left(kk, c):
        return hop(kk, c, 6, inner)

    goes_right = [
        (zz == 1) | ((zz == 0) & is_src),
        (zz == 1) | ((zz == 0) & is_src),
        ((zz == 1) & (ii == 0)) | ((zz == 0) & is_src),
        (zz == 0) & is_src,
    ]
    goes_left = [(zz == 1) & is_src] * 4
    goes = [goes_right[kk] | goes_left[kk] for kk in range(4)]

    ofam = 1 - y
    oz, ok = flip(z, 3, ofam), flip(row, 3, ofam)
    ways = [(oz == 2) & (ok == 3), oz == 2]

    def up(i2, c):
        return rc(slot(tr, i2, c), slot(pa, row, c), snd.at[10 + i2, c], sem_a.at[row, c], z, flip(jnp.int32(i2), 3, ofam))

    is_edge, is_inner = zz == 3, zz == 2
    not_edge = jnp.logical_not(is_edge)

    def b_far(c):
        return rc(part(b_ref, c), slot(pb, row, c), snd.at[12, c], sem_b.at[row, c], z, across)

    def b_near(c):
        return rc(part(b_ref, c), slot(pb, row, c), snd.at[13, c], sem_b.at[row, c], z, partner)

    def b_relay(c):
        return rc(slot(pb, across, c), slot(pb, across, c), snd.at[14, c], sem_b.at[across, c], z, partner)

    def e_own(c):
        return rc(part(b_ref, c), slot(pe, row, c), snd.at[13, c], sem_e.at[row, c], inner, row)

    def e_far(c):
        return rc(slot(pb, across, c), slot(pe, across, c), snd.at[14, c], sem_e.at[across, c], inner, row)

    def e_share(r, n, c):
        return rc(slot(pe, r, c), slot(pe, r, c), snd.at[n, c], sem_e.at[r, c], z, partner)

    def o_edge(c):
        return rc(buf.at[2 + c % 2], part(o_ref, c), snd.at[17, c], sem_o.at[c], outer, row)

    def o_own(c):
        return pltpu.make_async_copy(buf.at[c % 2], part(o_ref, c), out_sem.at[c % 2])

    def for_chunks(f):
        def body(c, _):
            f(c)
            return 0
        lax.fori_loop(0, CHUNKS, body, 0)

    cp_a = pltpu.make_async_copy(a_ref, pa.at[row], loc.at[0])
    cp_b = pltpu.make_async_copy(b_ref, pb.at[row], loc.at[1])

    @pl.when(own_home)
    def _():
        cp_a.start()

    cp_b.start()

    @pl.when(own_home)
    def _():
        cp_a.wait()

    cp_b.wait()

    def wait_a(kk, c):
        k = real(kk)

        @pl.when(jnp.logical_not(own_home & (k == row)))
        def _():
            wait_slot(pa, sem_a, k, c)

    forwards = [(NEAR_LAG, 0, (zz < 2) & is_src), (NEAR_LAG, 1, (zz < 2) & is_src)]
    forwards += [(CROSS_LAG, kk, (zz < 2) & is_src) for kk in (2, 3)]
    forwards += [(HOP_LAG, kk, (zz == 1) & (ii == 0)) for kk in (0, 1)]
    forwards += [(PASS_LAG, 2, (zz == 1) & (ii == 0))]

    def in_range(s, lag):
        return (s >= lag) & (s < CHUNKS + lag)

    b_lag = jnp.where(is_inner, INNER_LAG, B_LAG)
    sum_lag = jnp.where(is_inner, INNER_LAG + 1, SUM_LAG)

    def step(s, _):
        @pl.when(s < CHUNKS)
        def _():
            @pl.when(jnp.logical_not(own_home))
            def _():
                to_home(s).start()

            @pl.when(sends_far)
            def _():
                to_way(s).start()

            b_far(s).start()

            @pl.when(is_edge)
            def _():
                e_own(s).start()

            @pl.when(not_edge)
            def _():
                b_near(s).start()

        for lag, kk, who in forwards:
            @pl.when(in_range(s, lag) & who)
            def _():
                c = s - lag
                wait_a(kk, c)

                @pl.when(goes_right[kk])
                def _():
                    right(kk, c).start()

                @pl.when(goes_left[kk])
                def _():
                    left(kk, c).start()

        @pl.when(in_range(s, WAY_LAG))
        def _():
            c = s - WAY_LAG
            for i2 in range(2):
                @pl.when(ways[i2])
                def _():
                    wait_slot(tr, sem_tr, i2, c)
                    up(i2, c).start()

        @pl.when(in_range(s, EDGE_LAG) & is_edge)
        def _():
            c = s - EDGE_LAG
            wait_slot(pb, sem_b, across, c)
            e_far(c).start()

        @pl.when(in_range(s, b_lag) & not_edge)
        def _():
            c = s - b_lag
            wait_slot(pb, sem_b, across, c)
            b_relay(c).start()

        for r, n in ((row, 15), (across, 16)):
            @pl.when(in_range(s, INNER_LAG) & is_inner)
            def _():
                c = s - INNER_LAG
                wait_slot(pe, sem_e, r, c)
                e_share(r, n, c).start()

        @pl.when(in_range(s, sum_lag) & not_edge)
        def _():
            c = s - sum_lag
            for r in (partner, diagonal):
                wait_slot(pb, sem_b, r, c)
            for kk in range(4):
                @pl.when(jnp.logical_not(goes[kk]))
                def _():
                    wait_a(kk, c)

            @pl.when(is_inner)
            def _():
                for r in (partner, diagonal):
                    wait_slot(pe, sem_e, r, c)

                @pl.when(c >= 2)
                def _():
                    o_edge(c - 2).wait_send()

                def edge(h, _):
                    channel_sum(pa, pe, c * size + h, buf, (2 + c % 2, h))
                    return 0

                lax.fori_loop(0, size, edge, 0)
                o_edge(c).start()

            @pl.when(c >= 2)
            def _():
                o_own(c - 2).wait()

            def own(h, _):
                channel_sum(pa, pb, c * size + h, buf, (c % 2, h))
                return 0

            lax.fori_loop(0, size, own, 0)
            o_own(c).start()
        return 0

    lax.fori_loop(0, CHUNKS + max(SUM_LAG, INNER_LAG + 1), step, 0)

    @pl.when(not_edge)
    def _():
        for c in range(CHUNKS - 2, CHUNKS):
            o_own(c).wait()

    @pl.when(is_inner)
    def _():
        for c in range(CHUNKS - 2, CHUNKS):
            o_edge(c).wait_send()

    def drain(c):
        @pl.when(jnp.logical_not(own_home))
        def _():
            to_home(c).wait_send()

        @pl.when(sends_far)
        def _():
            to_way(c).wait_send()

        b_far(c).wait_send()

        @pl.when(not_edge)
        def _():
            b_near(c).wait_send()
            b_relay(c).wait_send()

        @pl.when(is_edge)
        def _():
            e_own(c).wait_send()
            e_far(c).wait_send()
            rc(buf.at[0], part(o_ref, c), snd.at[0, c], sem_o.at[c], z, row).wait_recv()

        @pl.when(is_inner)
        def _():
            e_share(row, 15, c).wait_send()
            e_share(across, 16, c).wait_send()

        for kk in range(4):
            @pl.when(goes_right[kk])
            def _():
                right(kk, c).wait_send()

            @pl.when(goes_left[kk])
            def _():
                left(kk, c).wait_send()

        for i2 in range(2):
            @pl.when(ways[i2])
            def _():
                up(i2, c).wait_send()

    for_chunks(drain)


def move(a, b):
    tile = (64, 3, 96, 128)
    any_spec = pl.BlockSpec(memory_space=pltpu.HBM)
    o, _ = pl.pallas_call(
        move_kernel,
        out_shape=[jax.ShapeDtypeStruct(tile, jnp.float32), jax.ShapeDtypeStruct((2,) + tile, jnp.bfloat16)],
        in_specs=[any_spec] * 2,
        out_specs=[any_spec] * 2,
        scratch_shapes=[pltpu.VMEM((4,) + tile, jnp.bfloat16)] * 3 + [
            pltpu.VMEM((4, 64 // CHUNKS, 3, 96, 128), jnp.float32),
            pltpu.SemaphoreType.DMA((4, CHUNKS)),
            pltpu.SemaphoreType.DMA((4, CHUNKS)),
            pltpu.SemaphoreType.DMA((4, CHUNKS)),
            pltpu.SemaphoreType.DMA((2, CHUNKS)),
            pltpu.SemaphoreType.DMA((CHUNKS,)),
            pltpu.SemaphoreType.DMA((18, CHUNKS)),
            pltpu.SemaphoreType.DMA((2,)),
            pltpu.SemaphoreType.DMA((2,)),
        ],
        compiler_params=pltpu.CompilerParams(has_side_effects=True, vmem_limit_bytes=67043328),
    )(a, b)
    return o


def finish_kernel(o_ref, z_ref, gin_ref, gout_ref, wg_ref, wo_ref, out_ref, gi_ref, go_ref, wg4_ref, wo8_ref):
    @pl.when(pl.program_id(0) == 0)
    def _():
        gi_ref[...] = jnp.broadcast_to(column(ids((64, 64), 0) == ids((64, 64), 1), gin_ref[...]), (64, 384))
        go_ref[...] = jnp.broadcast_to(column(ids((512, 64), 0) // 8 == ids((512, 64), 1), gout_ref[...]), (512, 128))
        t = pick(ids((256, 64), 0) % 64 == ids((256, 64), 1), wg_ref[...])
        t = jnp.concatenate([t] * 4, axis=1)
        same = ids((256, 256), 0) // 64 == ids((256, 256), 1) // 64
        wg4_ref[...] = jnp.where(same, t, 0.0).astype(jnp.bfloat16)
        t = pick(ids((512, 64), 0) % 64 == ids((512, 64), 1), wo_ref[...]).astype(jnp.bfloat16)
        wide = (ids((64, 512), 1) // 8 == ids((64, 512), 0)).astype(jnp.bfloat16)
        t = jnp.dot(t, wide, preferred_element_type=jnp.float32)
        same = ids((512, 512), 0) // 64 == ids((512, 512), 1) % 8
        wo8_ref[...] = jnp.where(same, t, 0.0).astype(jnp.bfloat16)

    normed = []
    for sec in range(3):
        v = norm_channels(o_ref[:, sec], 1.0, 0).reshape(512, 128) * go_ref[...]
        normed.append(v.astype(jnp.bfloat16))
    upd = jnp.dot(wo8_ref[...], jnp.concatenate(normed, axis=1), preferred_element_type=jnp.float32)
    z = lanes(z_ref[0], z_ref[1]).astype(jnp.float32)
    x = norm_channels(z, gi_ref[...][None], 1).astype(jnp.bfloat16).reshape(512, 384)
    gate = jnp.concatenate(
        [jnp.dot(wg4_ref[...], x[256 * s:256 * s + 256], preferred_element_type=jnp.float32) for s in range(2)], axis=0)
    res = (z.reshape(512, 384) + sigmoid(gate) * upd).astype(jnp.bfloat16).reshape(8, 64, 384)
    out_ref[0] = jnp.concatenate([res[:, :, :128], res[:, :, 256:320]], axis=2)
    out_ref[1] = jnp.concatenate([res[:, :, 128:256], res[:, :, 320:]], axis=2)


def finish(o, z, gin, gout, w_g, w_o):
    rows = pl.BlockSpec((2, 8, 64, 192), lambda i: (0, i, 0, 0))
    full = lambda i: (0, 0)
    out = pl.pallas_call(
        finish_kernel,
        grid=(12,),
        out_shape=jax.ShapeDtypeStruct((2, 96, 64, 192), jnp.bfloat16),
        in_specs=[
            pl.BlockSpec((64, 3, 8, 128), lambda i: (0, 0, i, 0)),
            rows,
            pl.BlockSpec((1, 64), full),
            pl.BlockSpec((1, 64), full),
            pl.BlockSpec((64, 64), full),
            pl.BlockSpec((64, 64), full),
        ],
        out_specs=rows,
        scratch_shapes=[
            pltpu.VMEM((64, 384), jnp.float32),
            pltpu.VMEM((512, 128), jnp.float32),
            pltpu.VMEM((256, 256), jnp.bfloat16),
            pltpu.VMEM((512, 512), jnp.bfloat16),
        ],
        compiler_params=pltpu.CompilerParams(vmem_limit_bytes=60 * 1024 * 1024),
    )(o, z.reshape(2, 96, 64, 192), gin, gout, w_g, w_o)
    return out.reshape(192, 64, 192)


def solution(mesh):
    tile_spec = P(('batch', 'row'), 'col', None)
    mask_spec = P(('batch', 'row'), 'col')
    replicated = P()

    def local_step(pair, mask, gin, w_l, w_lg, w_r, w_rg, w_g, gout, w_o):
        z = jnp.transpose(pair, (0, 2, 1))
        a, b = project(z, mask, gin[None], w_l, w_lg, w_r, w_rg)
        o = move(a, b)
        out = finish(o, z, gin[None], gout[None], w_g, w_o)
        return jnp.transpose(out, (0, 2, 1))

    return jax.shard_map(local_step, mesh=mesh, in_specs=(tile_spec, mask_spec) + (replicated,) * 8, out_specs=tile_spec, check_vma=False)
```

```python
import jax
import jax.numpy as jnp
from jax import lax
from jax.experimental import pallas as pl
from jax.experimental.pallas import tpu as pltpu
from jax.sharding import PartitionSpec as P

LN_EPS = 0.00001
MESH = pl.DeviceIdType.MESH
CHUNKS = 32
NEAR_LAG = 0
CROSS_LAG = 1
HOP_LAG = 1
PASS_LAG = 2
WAY_LAG = 1
B_LAG = 1
EDGE_LAG = 1
SUM_LAG = 4
INNER_LAG = 3


def sigmoid(v):
    return 0.5 * jnp.tanh(0.5 * v) + 0.5


def norm_channels(v, gain, axis):
    mean = jnp.mean(v, axis=axis, keepdims=True)
    cen = v - mean
    var = jnp.mean(cen * cen, axis=axis, keepdims=True)
    return cen * lax.rsqrt(var + LN_EPS) * gain


def lanes(p, q):
    return jnp.concatenate([p[..., :128], q[..., :128], p[..., 128:], q[..., 128:]], axis=-1)


def ids(shape, axis):
    return lax.broadcasted_iota(jnp.int32, shape, axis)


def pick(sel, w):
    return lax.dot_general(sel.astype(jnp.bfloat16), w, (((1,), (1,)), ((), ())), preferred_element_type=jnp.float32)


def column(sel, row):
    return jnp.sum(jnp.where(sel, row.astype(jnp.float32), 0.0), axis=1, keepdims=True)


def project_kernel(z_ref, m_ref, gin_ref, wl_ref, wlg_ref, wr_ref, wrg_ref, a_ref, b_ref, gain_ref, we_ref, wo_ref):
    @pl.when(pl.program_id(0) == 0)
    def _():
        gain_ref[...] = jnp.broadcast_to(column(ids((64, 64), 0) == ids((64, 64), 1), gin_ref[...]), (64, 384))
        chan = ids((256, 64), 0) // 4
        diag = ids((256, 256), 0) % 4 == ids((256, 256), 1) // 64
        for dst, sel in ((we_ref, chan == ids((256, 64), 1)), (wo_ref, chan == (ids((256, 64), 1) ^ 1))):
            for n, w_ref in enumerate((wl_ref, wlg_ref, wr_ref, wrg_ref)):
                t = pick(sel, w_ref[...])
                t = jnp.concatenate([t] * 4, axis=1)
                dst[256 * n:256 * n + 256, :] = jnp.where(diag, t, 0.0).astype(jnp.bfloat16)

    gain = gain_ref[...][None]
    low = ids((32, 8, 384), 1) < 4
    for half in range(2):
        acts = []
        for par, w_ref in ((0, we_ref), (1, wo_ref)):
            r = 16 * half + 4 * par
            z = lanes(z_ref[r:r + 4], z_ref[r + 8:r + 12]).astype(jnp.float32)
            rhs = norm_channels(z, gain, 1).astype(jnp.bfloat16).reshape(256, 384)
            keep = lanes(m_ref[r:r + 4].astype(jnp.float32), m_ref[r + 8:r + 12].astype(jnp.float32))
            keep = jnp.concatenate([keep, keep], axis=0)[None]
            proj = jnp.dot(w_ref[...], rhs, preferred_element_type=jnp.float32)
            proj = proj.reshape(4, 32, 8, 384)
            acts.append((keep * sigmoid(proj[1]) * proj[0], keep * sigmoid(proj[3]) * proj[2]))
        for e, o, ref in ((acts[0][0], acts[1][0], a_ref), (acts[0][1], acts[1][1], b_ref)):
            first = jnp.where(low, e, o)
            second = jnp.where(low, o, e)
            both = jnp.stack([first, second], axis=1).reshape(64, 8, 384).astype(jnp.bfloat16)
            for sec in range(3):
                ref[:, sec, 8 * half:8 * half + 8, :] = both[:, :, 128 * sec:128 * sec + 128]


def project(z, m, gin, w_l, w_lg, w_r, w_rg):
    full = lambda i: (0, 0)
    tile = jax.ShapeDtypeStruct((64, 3, 96, 128), jnp.bfloat16)
    out_spec = pl.BlockSpec((64, 3, 16, 128), lambda i: (0, 0, i, 0))
    return pl.pallas_call(
        project_kernel,
        grid=(6,),
        out_shape=[tile, tile],
        in_specs=[
            pl.BlockSpec((32, 64, 192), lambda i: (i, 0, 0)),
            pl.BlockSpec((32, 192), lambda i: (i, 0)),
            pl.BlockSpec((1, 64), full),
        ] + [pl.BlockSpec((64, 64), full)] * 4,
        out_specs=[out_spec, out_spec],
        scratch_shapes=[
            pltpu.VMEM((64, 384), jnp.float32),
            pltpu.VMEM((1024, 256), jnp.bfloat16),
            pltpu.VMEM((1024, 256), jnp.bfloat16),
        ],
        compiler_params=pltpu.CompilerParams(vmem_limit_bytes=60 * 1024 * 1024),
    )(z, m, gin, w_l, w_lg, w_r, w_rg)


def channel_sum(pa, pb, h, buf, at):
    def sides(ref):
        sec = [ref[:, h, s].reshape(384, 128) for s in range(3)]
        return jnp.concatenate([sec[0], sec[2]], axis=1), jnp.concatenate([sec[1], sec[2]], axis=1)

    a_lo, a_hi = sides(pa)
    b_lo, b_hi = sides(pb)
    dims = (((0,), (0,)), ((), ()))
    lo = lax.dot_general(a_lo, b_lo, dims, preferred_element_type=jnp.float32)
    hi = lax.dot_general(a_hi, b_hi, dims, preferred_element_type=jnp.float32)
    wide = jnp.concatenate([lo[0:128, 0:128] + hi[0:128, 0:128], lo[128:192, 0:128] + hi[192:256, 0:128]], axis=0)
    rest = jnp.concatenate(
        [lo[0:128, 128:192] + hi[0:128, 192:256], lo[128:192, 128:192] + lo[192:256, 192:256]], axis=0)
    buf[at + (0,)] = wide[0:96]
    buf[at + (1,)] = wide[96:192]
    buf[at + (2,)] = jnp.concatenate([rest[0:96], rest[96:192]], axis=1)


def move_kernel(a_ref, b_ref, o_ref, tr, pa, pb, pe, buf, sem_a, sem_b, sem_e, sem_tr, sem_o, snd, loc, out_sem):
    bat, z, row = lax.axis_index('batch'), lax.axis_index('col'), lax.axis_index('row')
    y, core = row // 2, row % 2
    size = 64 // CHUNKS

    def flip(v, n, fam):
        return jnp.where(fam == 0, v, n - v)

    def dev(col, r):
        return {'batch': bat, 'col': col, 'row': r}

    def rc(src, dst, send, recv, col, r):
        return pltpu.make_async_remote_copy(
            src_ref=src, dst_ref=dst, send_sem=send, recv_sem=recv, device_id=dev(col, r), device_id_type=MESH)

    def part(ref, c):
        return ref.at[pl.ds(c * size, size)]

    def slot(ref, s, c):
        return ref.at[s, pl.ds(c * size, size)]

    def wait_slot(ref, sem, s, c):
        rc(slot(ref, s, c), slot(ref, s, c), snd.at[0, c], sem.at[s, c], z, row).wait_recv()

    partner, across = 2 * y + 1 - core, 2 * (1 - y) + core
    diagonal = 2 * (1 - y) + 1 - core

    fam = z // 2
    blk = flip(z, 3, fam)
    home = y == fam
    k_src = flip(row, 3, fam)
    own_home = home & (row == z)
    sends_far = jnp.logical_not(home) & ((k_src == 3) | (blk == 1))

    def to_home(c):
        return rc(part(a_ref, c), slot(pa, row, c), snd.at[0, c], sem_a.at[row, c], z, z)

    def to_way(c):
        return rc(part(a_ref, c), slot(tr, blk, c), snd.at[1, c], sem_tr.at[blk, c], flip(jnp.int32(2), 3, fam), row)

    zz, ii = flip(z, 3, y), flip(row, 3, y)
    is_src = ii == zz
    inner = jnp.where(y == 0, z - 1, z + 1)
    outer = jnp.where(y == 0, z + 1, z - 1)

    def real(kk):
        return flip(jnp.int32(kk), 3, y)

    def hop(kk, c, n, col):
        k = real(kk)
        return rc(slot(pa, k, c), slot(pa, k, c), snd.at[n + kk, c], sem_a.at[k, c], col, row)

    def right(kk, c):
        return hop(kk, c, 2, outer)

    def left(kk, c):
        return hop(kk, c, 6, inner)

    goes_right = [
        (zz == 1) | ((zz == 0) & is_src),
        (zz == 1) | ((zz == 0) & is_src),
        ((zz == 1) & (ii == 0)) | ((zz == 0) & is_src),
        (zz == 0) & is_src,
    ]
    goes_left = [(zz == 1) & is_src] * 4
    goes = [goes_right[kk] | goes_left[kk] for kk in range(4)]

    ofam = 1 - y
    oz, ok = flip(z, 3, ofam), flip(row, 3, ofam)
    ways = [(oz == 2) & (ok == 3), oz == 2]

    def up(i2, c):
        return rc(slot(tr, i2, c), slot(pa, row, c), snd.at[10 + i2, c], sem_a.at[row, c], z, flip(jnp.int32(i2), 3, ofam))

    is_edge, is_inner = zz == 3, zz == 2
    not_edge = jnp.logical_not(is_edge)

    def b_far(c):
        return rc(part(b_ref, c), slot(pb, row, c), snd.at[12, c], sem_b.at[row, c], z, across)

    def b_near(c):
        return rc(part(b_ref, c), slot(pb, row, c), snd.at[13, c], sem_b.at[row, c], z, partner)

    def b_relay(c):
        return rc(slot(pb, across, c), slot(pb, across, c), snd.at[14, c], sem_b.at[across, c], z, partner)

    def e_own(c):
        return rc(part(b_ref, c), slot(pe, row, c), snd.at[13, c], sem_e.at[row, c], inner, row)

    def e_far(c):
        return rc(slot(pb, across, c), slot(pe, across, c), snd.at[14, c], sem_e.at[across, c], inner, row)

    def e_share(r, n, c):
        return rc(slot(pe, r, c), slot(pe, r, c), snd.at[n, c], sem_e.at[r, c], z, partner)

    def o_edge(c):
        return rc(buf.at[2 + c % 2], part(o_ref, c), snd.at[17, c], sem_o.at[c], outer, row)

    def o_own(c):
        return pltpu.make_async_copy(buf.at[c % 2], part(o_ref, c), out_sem.at[c % 2])

    def for_chunks(f):
        def body(c, _):
            f(c)
            return 0
        lax.fori_loop(0, CHUNKS, body, 0)

    cp_a = pltpu.make_async_copy(a_ref, pa.at[row], loc.at[0])
    cp_b = pltpu.make_async_copy(b_ref, pb.at[row], loc.at[1])

    @pl.when(own_home)
    def _():
        cp_a.start()

    cp_b.start()

    @pl.when(own_home)
    def _():
        cp_a.wait()

    cp_b.wait()

    def wait_a(kk, c):
        k = real(kk)

        @pl.when(jnp.logical_not(own_home & (k == row)))
        def _():
            wait_slot(pa, sem_a, k, c)

    forwards = [(NEAR_LAG, 0, (zz < 2) & is_src), (NEAR_LAG, 1, (zz < 2) & is_src)]
    forwards += [(CROSS_LAG, kk, (zz < 2) & is_src) for kk in (2, 3)]
    forwards += [(HOP_LAG, kk, (zz == 1) & (ii == 0)) for kk in (0, 1)]
    forwards += [(PASS_LAG, 2, (zz == 1) & (ii == 0))]

    def in_range(s, lag):
        return (s >= lag) & (s < CHUNKS + lag)

    b_lag = jnp.where(is_inner, INNER_LAG, B_LAG)
    sum_lag = jnp.where(is_inner, INNER_LAG + 1, SUM_LAG)

    def step(s, _):
        for lag, kk, who in forwards:
            @pl.when(in_range(s, lag) & who)
            def _():
                c = s - lag
                wait_a(kk, c)

                @pl.when(goes_right[kk])
                def _():
                    right(kk, c).start()

                @pl.when(goes_left[kk])
                def _():
                    left(kk, c).start()

        @pl.when(s < CHUNKS)
        def _():
            @pl.when(jnp.logical_not(own_home))
            def _():
                to_home(s).start()

            @pl.when(sends_far)
            def _():
                to_way(s).start()

            b_far(s).start()

            @pl.when(is_edge)
            def _():
                e_own(s).start()

            @pl.when(not_edge)
            def _():
                b_near(s).start()

        @pl.when(in_range(s, WAY_LAG))
        def _():
            c = s - WAY_LAG
            for i2 in range(2):
                @pl.when(ways[i2])
                def _():
                    wait_slot(tr, sem_tr, i2, c)
                    up(i2, c).start()

        @pl.when(in_range(s, EDGE_LAG) & is_edge)
        def _():
            c = s - EDGE_LAG
            wait_slot(pb, sem_b, across, c)
            e_far(c).start()

        @pl.when(in_range(s, b_lag) & not_edge)
        def _():
            c = s - b_lag
            wait_slot(pb, sem_b, across, c)
            b_relay(c).start()

        for r, n in ((row, 15), (across, 16)):
            @pl.when(in_range(s, INNER_LAG) & is_inner)
            def _():
                c = s - INNER_LAG
                wait_slot(pe, sem_e, r, c)
                e_share(r, n, c).start()

        @pl.when(in_range(s, sum_lag) & not_edge)
        def _():
            c = s - sum_lag
            for r in (partner, diagonal):
                wait_slot(pb, sem_b, r, c)
            for kk in range(4):
                @pl.when(jnp.logical_not(goes[kk]))
                def _():
                    wait_a(kk, c)

            @pl.when(is_inner)
            def _():
                for r in (partner, diagonal):
                    wait_slot(pe, sem_e, r, c)

                @pl.when(c >= 2)
                def _():
                    o_edge(c - 2).wait_send()

                def edge(h, _):
                    channel_sum(pa, pe, c * size + h, buf, (2 + c % 2, h))
                    return 0

                lax.fori_loop(0, size, edge, 0)
                o_edge(c).start()

            @pl.when(c >= 2)
            def _():
                o_own(c - 2).wait()

            def own(h, _):
                channel_sum(pa, pb, c * size + h, buf, (c % 2, h))
                return 0

            lax.fori_loop(0, size, own, 0)
            o_own(c).start()
        return 0

    lax.fori_loop(0, CHUNKS + max(SUM_LAG, INNER_LAG + 1), step, 0)

    @pl.when(not_edge)
    def _():
        for c in range(CHUNKS - 2, CHUNKS):
            o_own(c).wait()

    @pl.when(is_inner)
    def _():
        for c in range(CHUNKS - 2, CHUNKS):
            o_edge(c).wait_send()

    def drain(c):
        @pl.when(jnp.logical_not(own_home))
        def _():
            to_home(c).wait_send()

        @pl.when(sends_far)
        def _():
            to_way(c).wait_send()

        b_far(c).wait_send()

        @pl.when(not_edge)
        def _():
            b_near(c).wait_send()
            b_relay(c).wait_send()

        @pl.when(is_edge)
        def _():
            e_own(c).wait_send()
            e_far(c).wait_send()
            rc(buf.at[0], part(o_ref, c), snd.at[0, c], sem_o.at[c], z, row).wait_recv()

        @pl.when(is_inner)
        def _():
            e_share(row, 15, c).wait_send()
            e_share(across, 16, c).wait_send()

        for kk in range(4):
            @pl.when(goes_right[kk])
            def _():
                right(kk, c).wait_send()

            @pl.when(goes_left[kk])
            def _():
                left(kk, c).wait_send()

        for i2 in range(2):
            @pl.when(ways[i2])
            def _():
                up(i2, c).wait_send()

    for_chunks(drain)


def move(a, b):
    tile = (64, 3, 96, 128)
    any_spec = pl.BlockSpec(memory_space=pltpu.HBM)
    o, _ = pl.pallas_call(
        move_kernel,
        out_shape=[jax.ShapeDtypeStruct(tile, jnp.float32), jax.ShapeDtypeStruct((2,) + tile, jnp.bfloat16)],
        in_specs=[any_spec] * 2,
        out_specs=[any_spec] * 2,
        scratch_shapes=[pltpu.VMEM((4,) + tile, jnp.bfloat16)] * 3 + [
            pltpu.VMEM((4, 64 // CHUNKS, 3, 96, 128), jnp.float32),
            pltpu.SemaphoreType.DMA((4, CHUNKS)),
            pltpu.SemaphoreType.DMA((4, CHUNKS)),
            pltpu.SemaphoreType.DMA((4, CHUNKS)),
            pltpu.SemaphoreType.DMA((2, CHUNKS)),
            pltpu.SemaphoreType.DMA((CHUNKS,)),
            pltpu.SemaphoreType.DMA((18, CHUNKS)),
            pltpu.SemaphoreType.DMA((2,)),
            pltpu.SemaphoreType.DMA((2,)),
        ],
        compiler_params=pltpu.CompilerParams(has_side_effects=True, vmem_limit_bytes=67043328),
    )(a, b)
    return o


def finish_kernel(o_ref, z_ref, gin_ref, gout_ref, wg_ref, wo_ref, out_ref, gi_ref, go_ref, wg4_ref, wo8_ref):
    @pl.when(pl.program_id(0) == 0)
    def _():
        gi_ref[...] = jnp.broadcast_to(column(ids((64, 64), 0) == ids((64, 64), 1), gin_ref[...]), (64, 384))
        go_ref[...] = jnp.broadcast_to(column(ids((512, 64), 0) // 8 == ids((512, 64), 1), gout_ref[...]), (512, 128))
        t = pick(ids((256, 64), 0) % 64 == ids((256, 64), 1), wg_ref[...])
        t = jnp.concatenate([t] * 4, axis=1)
        same = ids((256, 256), 0) // 64 == ids((256, 256), 1) // 64
        wg4_ref[...] = jnp.where(same, t, 0.0).astype(jnp.bfloat16)
        t = pick(ids((512, 64), 0) % 64 == ids((512, 64), 1), wo_ref[...]).astype(jnp.bfloat16)
        wide = (ids((64, 512), 1) // 8 == ids((64, 512), 0)).astype(jnp.bfloat16)
        t = jnp.dot(t, wide, preferred_element_type=jnp.float32)
        same = ids((512, 512), 0) // 64 == ids((512, 512), 1) % 8
        wo8_ref[...] = jnp.where(same, t, 0.0).astype(jnp.bfloat16)

    normed = []
    for sec in range(3):
        v = norm_channels(o_ref[:, sec], 1.0, 0).reshape(512, 128) * go_ref[...]
        normed.append(v.astype(jnp.bfloat16))
    upd = jnp.dot(wo8_ref[...], jnp.concatenate(normed, axis=1), preferred_element_type=jnp.float32)
    z = lanes(z_ref[0], z_ref[1]).astype(jnp.float32)
    x = norm_channels(z, gi_ref[...][None], 1).astype(jnp.bfloat16).reshape(512, 384)
    gate = jnp.concatenate(
        [jnp.dot(wg4_ref[...], x[256 * s:256 * s + 256], preferred_element_type=jnp.float32) for s in range(2)], axis=0)
    res = (z.reshape(512, 384) + sigmoid(gate) * upd).astype(jnp.bfloat16).reshape(8, 64, 384)
    out_ref[0] = jnp.concatenate([res[:, :, :128], res[:, :, 256:320]], axis=2)
    out_ref[1] = jnp.concatenate([res[:, :, 128:256], res[:, :, 320:]], axis=2)


def finish(o, z, gin, gout, w_g, w_o):
    rows = pl.BlockSpec((2, 8, 64, 192), lambda i: (0, i, 0, 0))
    full = lambda i: (0, 0)
    out = pl.pallas_call(
        finish_kernel,
        grid=(12,),
        out_shape=jax.ShapeDtypeStruct((2, 96, 64, 192), jnp.bfloat16),
        in_specs=[
            pl.BlockSpec((64, 3, 8, 128), lambda i: (0, 0, i, 0)),
            rows,
            pl.BlockSpec((1, 64), full),
            pl.BlockSpec((1, 64), full),
            pl.BlockSpec((64, 64), full),
            pl.BlockSpec((64, 64), full),
        ],
        out_specs=rows,
        scratch_shapes=[
            pltpu.VMEM((64, 384), jnp.float32),
            pltpu.VMEM((512, 128), jnp.float32),
            pltpu.VMEM((256, 256), jnp.bfloat16),
            pltpu.VMEM((512, 512), jnp.bfloat16),
        ],
        compiler_params=pltpu.CompilerParams(vmem_limit_bytes=60 * 1024 * 1024),
    )(o, z.reshape(2, 96, 64, 192), gin, gout, w_g, w_o)
    return out.reshape(192, 64, 192)


def solution(mesh):
    tile_spec = P(('batch', 'row'), 'col', None)
    mask_spec = P(('batch', 'row'), 'col')
    replicated = P()

    def local_step(pair, mask, gin, w_l, w_lg, w_r, w_rg, w_g, gout, w_o):
        z = jnp.transpose(pair, (0, 2, 1))
        a, b = project(z, mask, gin[None], w_l, w_lg, w_r, w_rg)
        o = move(a, b)
        out = finish(o, z, gin[None], gout[None], w_g, w_o)
        return jnp.transpose(out, (0, 2, 1))

    return jax.shard_map(local_step, mesh=mesh, in_specs=(tile_spec, mask_spec) + (replicated,) * 8, out_specs=tile_spec, check_vma=False)
```

```python
import jax
import jax.numpy as jnp
from jax import lax
from jax.experimental import pallas as pl
from jax.experimental.pallas import tpu as pltpu
from jax.sharding import PartitionSpec as P

LN_EPS = 0.00001
MESH = pl.DeviceIdType.MESH
CHUNKS = 32
NEAR_LAG = 0
CROSS_LAG = 1
HOP_LAG = 1
PASS_LAG = 2
WAY_LAG = 1
B_LAG = 1
EDGE_LAG = 1
SUM_LAG = 4
INNER_LAG = 2


def sigmoid(v):
    return 0.5 * jnp.tanh(0.5 * v) + 0.5


def norm_channels(v, gain, axis):
    mean = jnp.mean(v, axis=axis, keepdims=True)
    cen = v - mean
    var = jnp.mean(cen * cen, axis=axis, keepdims=True)
    return cen * lax.rsqrt(var + LN_EPS) * gain


def lanes(p, q):
    return jnp.concatenate([p[..., :128], q[..., :128], p[..., 128:], q[..., 128:]], axis=-1)


def ids(shape, axis):
    return lax.broadcasted_iota(jnp.int32, shape, axis)


def pick(sel, w):
    return lax.dot_general(sel.astype(jnp.bfloat16), w, (((1,), (1,)), ((), ())), preferred_element_type=jnp.float32)


def column(sel, row):
    return jnp.sum(jnp.where(sel, row.astype(jnp.float32), 0.0), axis=1, keepdims=True)


def project_kernel(z_ref, m_ref, gin_ref, wl_ref, wlg_ref, wr_ref, wrg_ref, a_ref, b_ref, gain_ref, we_ref, wo_ref):
    @pl.when(pl.program_id(0) == 0)
    def _():
        gain_ref[...] = jnp.broadcast_to(column(ids((64, 64), 0) == ids((64, 64), 1), gin_ref[...]), (64, 384))
        chan = ids((256, 64), 0) // 4
        diag = ids((256, 256), 0) % 4 == ids((256, 256), 1) // 64
        for dst, sel in ((we_ref, chan == ids((256, 64), 1)), (wo_ref, chan == (ids((256, 64), 1) ^ 1))):
            for n, w_ref in enumerate((wl_ref, wlg_ref, wr_ref, wrg_ref)):
                t = pick(sel, w_ref[...])
                t = jnp.concatenate([t] * 4, axis=1)
                dst[256 * n:256 * n + 256, :] = jnp.where(diag, t, 0.0).astype(jnp.bfloat16)

    gain = gain_ref[...][None]
    low = ids((32, 8, 384), 1) < 4
    for half in range(2):
        acts = []
        for par, w_ref in ((0, we_ref), (1, wo_ref)):
            r = 16 * half + 4 * par
            z = lanes(z_ref[r:r + 4], z_ref[r + 8:r + 12]).astype(jnp.float32)
            rhs = norm_channels(z, gain, 1).astype(jnp.bfloat16).reshape(256, 384)
            keep = lanes(m_ref[r:r + 4].astype(jnp.float32), m_ref[r + 8:r + 12].astype(jnp.float32))
            keep = jnp.concatenate([keep, keep], axis=0)[None]
            proj = jnp.dot(w_ref[...], rhs, preferred_element_type=jnp.float32)
            proj = proj.reshape(4, 32, 8, 384)
            acts.append((keep * sigmoid(proj[1]) * proj[0], keep * sigmoid(proj[3]) * proj[2]))
        for e, o, ref in ((acts[0][0], acts[1][0], a_ref), (acts[0][1], acts[1][1], b_ref)):
            first = jnp.where(low, e, o)
            second = jnp.where(low, o, e)
            both = jnp.stack([first, second], axis=1).reshape(64, 8, 384).astype(jnp.bfloat16)
            for sec in range(3):
                ref[:, sec, 8 * half:8 * half + 8, :] = both[:, :, 128 * sec:128 * sec + 128]


def project(z, m, gin, w_l, w_lg, w_r, w_rg):
    full = lambda i: (0, 0)
    tile = jax.ShapeDtypeStruct((64, 3, 96, 128), jnp.bfloat16)
    out_spec = pl.BlockSpec((64, 3, 16, 128), lambda i: (0, 0, i, 0))
    return pl.pallas_call(
        project_kernel,
        grid=(6,),
        out_shape=[tile, tile],
        in_specs=[
            pl.BlockSpec((32, 64, 192), lambda i: (i, 0, 0)),
            pl.BlockSpec((32, 192), lambda i: (i, 0)),
            pl.BlockSpec((1, 64), full),
        ] + [pl.BlockSpec((64, 64), full)] * 4,
        out_specs=[out_spec, out_spec],
        scratch_shapes=[
            pltpu.VMEM((64, 384), jnp.float32),
            pltpu.VMEM((1024, 256), jnp.bfloat16),
            pltpu.VMEM((1024, 256), jnp.bfloat16),
        ],
        compiler_params=pltpu.CompilerParams(vmem_limit_bytes=60 * 1024 * 1024),
    )(z, m, gin, w_l, w_lg, w_r, w_rg)


def channel_sum(pa, pb, h, buf, at):
    def sides(ref):
        sec = [ref[:, h, s].reshape(384, 128) for s in range(3)]
        return jnp.concatenate([sec[0], sec[2]], axis=1), jnp.concatenate([sec[1], sec[2]], axis=1)

    a_lo, a_hi = sides(pa)
    b_lo, b_hi = sides(pb)
    dims = (((0,), (0,)), ((), ()))
    lo = lax.dot_general(a_lo, b_lo, dims, preferred_element_type=jnp.float32)
    hi = lax.dot_general(a_hi, b_hi, dims, preferred_element_type=jnp.float32)
    wide = jnp.concatenate([lo[0:128, 0:128] + hi[0:128, 0:128], lo[128:192, 0:128] + hi[192:256, 0:128]], axis=0)
    rest = jnp.concatenate(
        [lo[0:128, 128:192] + hi[0:128, 192:256], lo[128:192, 128:192] + lo[192:256, 192:256]], axis=0)
    buf[at + (0,)] = wide[0:96]
    buf[at + (1,)] = wide[96:192]
    buf[at + (2,)] = jnp.concatenate([rest[0:96], rest[96:192]], axis=1)


def move_kernel(a_ref, b_ref, o_ref, tr, pa, pb, pe, buf, sem_a, sem_b, sem_e, sem_tr, sem_o, snd, loc, out_sem):
    bat, z, row = lax.axis_index('batch'), lax.axis_index('col'), lax.axis_index('row')
    y, core = row // 2, row % 2
    size = 64 // CHUNKS

    def flip(v, n, fam):
        return jnp.where(fam == 0, v, n - v)

    def dev(col, r):
        return {'batch': bat, 'col': col, 'row': r}

    def rc(src, dst, send, recv, col, r):
        return pltpu.make_async_remote_copy(
            src_ref=src, dst_ref=dst, send_sem=send, recv_sem=recv, device_id=dev(col, r), device_id_type=MESH)

    def part(ref, c):
        return ref.at[pl.ds(c * size, size)]

    def slot(ref, s, c):
        return ref.at[s, pl.ds(c * size, size)]

    def wait_slot(ref, sem, s, c):
        rc(slot(ref, s, c), slot(ref, s, c), snd.at[0, c], sem.at[s, c], z, row).wait_recv()

    partner, across = 2 * y + 1 - core, 2 * (1 - y) + core
    diagonal = 2 * (1 - y) + 1 - core

    fam = z // 2
    blk = flip(z, 3, fam)
    home = y == fam
    k_src = flip(row, 3, fam)
    own_home = home & (row == z)
    sends_far = jnp.logical_not(home) & ((k_src == 3) | (blk == 1))

    def to_home(c):
        return rc(part(a_ref, c), slot(pa, row, c), snd.at[0, c], sem_a.at[row, c], z, z)

    def to_way(c):
        return rc(part(a_ref, c), slot(tr, blk, c), snd.at[1, c], sem_tr.at[blk, c], flip(jnp.int32(2), 3, fam), row)

    zz, ii = flip(z, 3, y), flip(row, 3, y)
    is_src = ii == zz
    inner = jnp.where(y == 0, z - 1, z + 1)
    outer = jnp.where(y == 0, z + 1, z - 1)

    def real(kk):
        return flip(jnp.int32(kk), 3, y)

    def hop(kk, c, n, col):
        k = real(kk)
        return rc(slot(pa, k, c), slot(pa, k, c), snd.at[n + kk, c], sem_a.at[k, c], col, row)

    def right(kk, c):
        return hop(kk, c, 2, outer)

    def left(kk, c):
        return hop(kk, c, 6, inner)

    goes_right = [
        (zz == 1) | ((zz == 0) & is_src),
        (zz == 1) | ((zz == 0) & is_src),
        ((zz == 1) & (ii == 0)) | ((zz == 0) & is_src),
        (zz == 0) & is_src,
    ]
    goes_left = [(zz == 1) & is_src] * 4
    goes = [goes_right[kk] | goes_left[kk] for kk in range(4)]

    ofam = 1 - y
    oz, ok = flip(z, 3, ofam), flip(row, 3, ofam)
    ways = [(oz == 2) & (ok == 3), oz == 2]

    def up(i2, c):
        return rc(slot(tr, i2, c), slot(pa, row, c), snd.at[10 + i2, c], sem_a.at[row, c], z, flip(jnp.int32(i2), 3, ofam))

    is_edge, is_inner = zz == 3, zz == 2
    not_edge = jnp.logical_not(is_edge)

    def b_far(c):
        return rc(part(b_ref, c), slot(pb, row, c), snd.at[12, c], sem_b.at[row, c], z, across)

    def b_near(c):
        return rc(part(b_ref, c), slot(pb, row, c), snd.at[13, c], sem_b.at[row, c], z, partner)

    def b_relay(c):
        return rc(slot(pb, across, c), slot(pb, across, c), snd.at[14, c], sem_b.at[across, c], z, partner)

    def e_own(c):
        return rc(part(b_ref, c), slot(pe, row, c), snd.at[13, c], sem_e.at[row, c], inner, row)

    def e_far(c):
        return rc(slot(pb, across, c), slot(pe, across, c), snd.at[14, c], sem_e.at[across, c], inner, row)

    def e_share(r, n, c):
        return rc(slot(pe, r, c), slot(pe, r, c), snd.at[n, c], sem_e.at[r, c], z, partner)

    def o_edge(c):
        return rc(buf.at[2 + c % 2], part(o_ref, c), snd.at[17, c], sem_o.at[c], outer, row)

    def o_own(c):
        return pltpu.make_async_copy(buf.at[c % 2], part(o_ref, c), out_sem.at[c % 2])

    def for_chunks(f):
        def body(c, _):
            f(c)
            return 0
        lax.fori_loop(0, CHUNKS, body, 0)

    cp_a = pltpu.make_async_copy(a_ref, pa.at[row], loc.at[0])
    cp_b = pltpu.make_async_copy(b_ref, pb.at[row], loc.at[1])

    @pl.when(own_home)
    def _():
        cp_a.start()

    cp_b.start()

    @pl.when(own_home)
    def _():
        cp_a.wait()

    cp_b.wait()

    def wait_a(kk, c):
        k = real(kk)

        @pl.when(jnp.logical_not(own_home & (k == row)))
        def _():
            wait_slot(pa, sem_a, k, c)

    forwards = [(NEAR_LAG, 0, (zz < 2) & is_src), (NEAR_LAG, 1, (zz < 2) & is_src)]
    forwards += [(CROSS_LAG, kk, (zz < 2) & is_src) for kk in (2, 3)]
    forwards += [(HOP_LAG, kk, (zz == 1) & (ii == 0)) for kk in (0, 1)]
    forwards += [(PASS_LAG, 2, (zz == 1) & (ii == 0))]

    def in_range(s, lag):
        return (s >= lag) & (s < CHUNKS + lag)

    b_lag = jnp.where(is_inner, INNER_LAG, B_LAG)
    sum_lag = jnp.where(is_inner, INNER_LAG + 1, SUM_LAG)

    def step(s, _):
        for lag, kk, who in forwards:
            @pl.when(in_range(s, lag) & who)
            def _():
                c = s - lag
                wait_a(kk, c)

                @pl.when(goes_right[kk])
                def _():
                    right(kk, c).start()

                @pl.when(goes_left[kk])
                def _():
                    left(kk, c).start()

        @pl.when(s < CHUNKS)
        def _():
            @pl.when(jnp.logical_not(own_home))
            def _():
                to_home(s).start()

            @pl.when(sends_far)
            def _():
                to_way(s).start()

            b_far(s).start()

            @pl.when(is_edge)
            def _():
                e_own(s).start()

            @pl.when(not_edge)
            def _():
                b_near(s).start()

        @pl.when(in_range(s, WAY_LAG))
        def _():
            c = s - WAY_LAG
            for i2 in range(2):
                @pl.when(ways[i2])
                def _():
                    wait_slot(tr, sem_tr, i2, c)
                    up(i2, c).start()

        @pl.when(in_range(s, EDGE_LAG) & is_edge)
        def _():
            c = s - EDGE_LAG
            wait_slot(pb, sem_b, across, c)
            e_far(c).start()

        @pl.when(in_range(s, b_lag) & not_edge)
        def _():
            c = s - b_lag
            wait_slot(pb, sem_b, across, c)
            b_relay(c).start()

        for r, n in ((row, 15), (across, 16)):
            @pl.when(in_range(s, INNER_LAG) & is_inner)
            def _():
                c = s - INNER_LAG
                wait_slot(pe, sem_e, r, c)
                e_share(r, n, c).start()

        @pl.when(in_range(s, sum_lag) & not_edge)
        def _():
            c = s - sum_lag
            for r in (partner, diagonal):
                wait_slot(pb, sem_b, r, c)
            for kk in range(4):
                @pl.when(jnp.logical_not(goes[kk]))
                def _():
                    wait_a(kk, c)

            @pl.when(is_inner)
            def _():
                for r in (partner, diagonal):
                    wait_slot(pe, sem_e, r, c)

                @pl.when(c >= 2)
                def _():
                    o_edge(c - 2).wait_send()

                def edge(h, _):
                    channel_sum(pa, pe, c * size + h, buf, (2 + c % 2, h))
                    return 0

                lax.fori_loop(0, size, edge, 0)
                o_edge(c).start()

            @pl.when(c >= 2)
            def _():
                o_own(c - 2).wait()

            def own(h, _):
                channel_sum(pa, pb, c * size + h, buf, (c % 2, h))
                return 0

            lax.fori_loop(0, size, own, 0)
            o_own(c).start()
        return 0

    lax.fori_loop(0, CHUNKS + max(SUM_LAG, INNER_LAG + 1), step, 0)

    @pl.when(not_edge)
    def _():
        for c in range(CHUNKS - 2, CHUNKS):
            o_own(c).wait()

    @pl.when(is_inner)
    def _():
        for c in range(CHUNKS - 2, CHUNKS):
            o_edge(c).wait_send()

    def drain(c):
        @pl.when(jnp.logical_not(own_home))
        def _():
            to_home(c).wait_send()

        @pl.when(sends_far)
        def _():
            to_way(c).wait_send()

        b_far(c).wait_send()

        @pl.when(not_edge)
        def _():
            b_near(c).wait_send()
            b_relay(c).wait_send()

        @pl.when(is_edge)
        def _():
            e_own(c).wait_send()
            e_far(c).wait_send()
            rc(buf.at[0], part(o_ref, c), snd.at[0, c], sem_o.at[c], z, row).wait_recv()

        @pl.when(is_inner)
        def _():
            e_share(row, 15, c).wait_send()
            e_share(across, 16, c).wait_send()

        for kk in range(4):
            @pl.when(goes_right[kk])
            def _():
                right(kk, c).wait_send()

            @pl.when(goes_left[kk])
            def _():
                left(kk, c).wait_send()

        for i2 in range(2):
            @pl.when(ways[i2])
            def _():
                up(i2, c).wait_send()

    for_chunks(drain)


def move(a, b):
    tile = (64, 3, 96, 128)
    any_spec = pl.BlockSpec(memory_space=pltpu.HBM)
    o, _ = pl.pallas_call(
        move_kernel,
        out_shape=[jax.ShapeDtypeStruct(tile, jnp.float32), jax.ShapeDtypeStruct((2,) + tile, jnp.bfloat16)],
        in_specs=[any_spec] * 2,
        out_specs=[any_spec] * 2,
        scratch_shapes=[pltpu.VMEM((4,) + tile, jnp.bfloat16)] * 3 + [
            pltpu.VMEM((4, 64 // CHUNKS, 3, 96, 128), jnp.float32),
            pltpu.SemaphoreType.DMA((4, CHUNKS)),
            pltpu.SemaphoreType.DMA((4, CHUNKS)),
            pltpu.SemaphoreType.DMA((4, CHUNKS)),
            pltpu.SemaphoreType.DMA((2, CHUNKS)),
            pltpu.SemaphoreType.DMA((CHUNKS,)),
            pltpu.SemaphoreType.DMA((18, CHUNKS)),
            pltpu.SemaphoreType.DMA((2,)),
            pltpu.SemaphoreType.DMA((2,)),
        ],
        compiler_params=pltpu.CompilerParams(has_side_effects=True, vmem_limit_bytes=67043328),
    )(a, b)
    return o


def finish_kernel(o_ref, z_ref, gin_ref, gout_ref, wg_ref, wo_ref, out_ref, gi_ref, go_ref, wg4_ref, wo8_ref):
    @pl.when(pl.program_id(0) == 0)
    def _():
        gi_ref[...] = jnp.broadcast_to(column(ids((64, 64), 0) == ids((64, 64), 1), gin_ref[...]), (64, 384))
        go_ref[...] = jnp.broadcast_to(column(ids((512, 64), 0) // 8 == ids((512, 64), 1), gout_ref[...]), (512, 128))
        t = pick(ids((256, 64), 0) % 64 == ids((256, 64), 1), wg_ref[...])
        t = jnp.concatenate([t] * 4, axis=1)
        same = ids((256, 256), 0) // 64 == ids((256, 256), 1) // 64
        wg4_ref[...] = jnp.where(same, t, 0.0).astype(jnp.bfloat16)
        t = pick(ids((512, 64), 0) % 64 == ids((512, 64), 1), wo_ref[...]).astype(jnp.bfloat16)
        wide = (ids((64, 512), 1) // 8 == ids((64, 512), 0)).astype(jnp.bfloat16)
        t = jnp.dot(t, wide, preferred_element_type=jnp.float32)
        same = ids((512, 512), 0) // 64 == ids((512, 512), 1) % 8
        wo8_ref[...] = jnp.where(same, t, 0.0).astype(jnp.bfloat16)

    for q in range(2):
        rows = slice(8 * q, 8 * q + 8)
        normed = []
        for sec in range(3):
            v = norm_channels(o_ref[:, sec, rows], 1.0, 0).reshape(512, 128) * go_ref[...]
            normed.append(v.astype(jnp.bfloat16))
        upd = jnp.dot(wo8_ref[...], jnp.concatenate(normed, axis=1), preferred_element_type=jnp.float32)
        z = lanes(z_ref[0, rows], z_ref[1, rows]).astype(jnp.float32)
        x = norm_channels(z, gi_ref[...][None], 1).astype(jnp.bfloat16).reshape(512, 384)
        gate = jnp.concatenate(
            [jnp.dot(wg4_ref[...], x[256 * s:256 * s + 256], preferred_element_type=jnp.float32) for s in range(2)], axis=0)
        res = (z.reshape(512, 384) + sigmoid(gate) * upd).astype(jnp.bfloat16).reshape(8, 64, 384)
        out_ref[0, rows] = jnp.concatenate([res[:, :, :128], res[:, :, 256:320]], axis=2)
        out_ref[1, rows] = jnp.concatenate([res[:, :, 128:256], res[:, :, 320:]], axis=2)


def finish(o, z, gin, gout, w_g, w_o):
    rows = pl.BlockSpec((2, 16, 64, 192), lambda i: (0, i, 0, 0))
    full = lambda i: (0, 0)
    out = pl.pallas_call(
        finish_kernel,
        grid=(6,),
        out_shape=jax.ShapeDtypeStruct((2, 96, 64, 192), jnp.bfloat16),
        in_specs=[
            pl.BlockSpec((64, 3, 16, 128), lambda i: (0, 0, i, 0)),
            rows,
            pl.BlockSpec((1, 64), full),
            pl.BlockSpec((1, 64), full),
            pl.BlockSpec((64, 64), full),
            pl.BlockSpec((64, 64), full),
        ],
        out_specs=rows,
        scratch_shapes=[
            pltpu.VMEM((64, 384), jnp.float32),
            pltpu.VMEM((512, 128), jnp.float32),
            pltpu.VMEM((256, 256), jnp.bfloat16),
            pltpu.VMEM((512, 512), jnp.bfloat16),
        ],
        compiler_params=pltpu.CompilerParams(vmem_limit_bytes=60 * 1024 * 1024),
    )(o, z.reshape(2, 96, 64, 192), gin, gout, w_g, w_o)
    return out.reshape(192, 64, 192)


def solution(mesh):
    tile_spec = P(('batch', 'row'), 'col', None)
    mask_spec = P(('batch', 'row'), 'col')
    replicated = P()

    def local_step(pair, mask, gin, w_l, w_lg, w_r, w_rg, w_g, gout, w_o):
        z = jnp.transpose(pair, (0, 2, 1))
        a, b = project(z, mask, gin[None], w_l, w_lg, w_r, w_rg)
        o = move(a, b)
        out = finish(o, z, gin[None], gout[None], w_g, w_o)
        return jnp.transpose(out, (0, 2, 1))

    return jax.shard_map(local_step, mesh=mesh, in_specs=(tile_spec, mask_spec) + (replicated,) * 8, out_specs=tile_spec, check_vma=False)
```

```python
import jax
import jax.numpy as jnp
from jax import lax
from jax.experimental import pallas as pl
from jax.experimental.pallas import tpu as pltpu
from jax.sharding import PartitionSpec as P

LN_EPS = 0.00001
MESH = pl.DeviceIdType.MESH
CHUNKS = 32
NEAR_LAG = 0
CROSS_LAG = 1
HOP_LAG = 1
PASS_LAG = 2
WAY_LAG = 1
B_LAG = 3
EDGE_LAG = 1
SUM_LAG = 8
INNER_LAG = 2


def sigmoid(v):
    return 0.5 * jnp.tanh(0.5 * v) + 0.5


def norm_channels(v, gain, axis):
    mean = jnp.mean(v, axis=axis, keepdims=True)
    cen = v - mean
    var = jnp.mean(cen * cen, axis=axis, keepdims=True)
    return cen * lax.rsqrt(var + LN_EPS) * gain


def lanes(p, q):
    return jnp.concatenate([p[..., :128], q[..., :128], p[..., 128:], q[..., 128:]], axis=-1)


def ids(shape, axis):
    return lax.broadcasted_iota(jnp.int32, shape, axis)


def pick(sel, w):
    return lax.dot_general(sel.astype(jnp.bfloat16), w, (((1,), (1,)), ((), ())), preferred_element_type=jnp.float32)


def column(sel, row):
    return jnp.sum(jnp.where(sel, row.astype(jnp.float32), 0.0), axis=1, keepdims=True)


def project_kernel(z_ref, m_ref, gin_ref, wl_ref, wlg_ref, wr_ref, wrg_ref, a_ref, b_ref, gain_ref, we_ref, wo_ref):
    @pl.when(pl.program_id(0) == 0)
    def _():
        gain_ref[...] = jnp.broadcast_to(column(ids((64, 64), 0) == ids((64, 64), 1), gin_ref[...]), (64, 384))
        chan = ids((256, 64), 0) // 4
        diag = ids((256, 256), 0) % 4 == ids((256, 256), 1) // 64
        for dst, sel in ((we_ref, chan == ids((256, 64), 1)), (wo_ref, chan == (ids((256, 64), 1) ^ 1))):
            for n, w_ref in enumerate((wl_ref, wlg_ref, wr_ref, wrg_ref)):
                t = pick(sel, w_ref[...])
                t = jnp.concatenate([t] * 4, axis=1)
                dst[256 * n:256 * n + 256, :] = jnp.where(diag, t, 0.0).astype(jnp.bfloat16)

    gain = gain_ref[...][None]
    low = ids((32, 8, 384), 1) < 4
    for half in range(2):
        acts = []
        for par, w_ref in ((0, we_ref), (1, wo_ref)):
            r = 16 * half + 4 * par
            z = lanes(z_ref[r:r + 4], z_ref[r + 8:r + 12]).astype(jnp.float32)
            rhs = norm_channels(z, gain, 1).astype(jnp.bfloat16).reshape(256, 384)
            keep = lanes(m_ref[r:r + 4].astype(jnp.float32), m_ref[r + 8:r + 12].astype(jnp.float32))
            keep = jnp.concatenate([keep, keep], axis=0)[None]
            proj = jnp.dot(w_ref[...], rhs, preferred_element_type=jnp.float32)
            proj = proj.reshape(4, 32, 8, 384)
            acts.append((keep * sigmoid(proj[1]) * proj[0], keep * sigmoid(proj[3]) * proj[2]))
        for e, o, ref in ((acts[0][0], acts[1][0], a_ref), (acts[0][1], acts[1][1], b_ref)):
            first = jnp.where(low, e, o)
            second = jnp.where(low, o, e)
            both = jnp.stack([first, second], axis=1).reshape(64, 8, 384).astype(jnp.bfloat16)
            for sec in range(3):
                ref[:, sec, 8 * half:8 * half + 8, :] = both[:, :, 128 * sec:128 * sec + 128]


def project(z, m, gin, w_l, w_lg, w_r, w_rg):
    full = lambda i: (0, 0)
    tile = jax.ShapeDtypeStruct((64, 3, 96, 128), jnp.bfloat16)
    out_spec = pl.BlockSpec((64, 3, 16, 128), lambda i: (0, 0, i, 0))
    return pl.pallas_call(
        project_kernel,
        grid=(6,),
        out_shape=[tile, tile],
        in_specs=[
            pl.BlockSpec((32, 64, 192), lambda i: (i, 0, 0)),
            pl.BlockSpec((32, 192), lambda i: (i, 0)),
            pl.BlockSpec((1, 64), full),
        ] + [pl.BlockSpec((64, 64), full)] * 4,
        out_specs=[out_spec, out_spec],
        scratch_shapes=[
            pltpu.VMEM((64, 384), jnp.float32),
            pltpu.VMEM((1024, 256), jnp.bfloat16),
            pltpu.VMEM((1024, 256), jnp.bfloat16),
        ],
        compiler_params=pltpu.CompilerParams(vmem_limit_bytes=60 * 1024 * 1024),
    )(z, m, gin, w_l, w_lg, w_r, w_rg)


def channel_sum(pa, pb, h, buf, at):
    def sides(ref):
        sec = [ref[:, h, s].reshape(384, 128) for s in range(3)]
        return jnp.concatenate([sec[0], sec[2]], axis=1), jnp.concatenate([sec[1], sec[2]], axis=1)

    a_lo, a_hi = sides(pa)
    b_lo, b_hi = sides(pb)
    dims = (((0,), (0,)), ((), ()))
    lo = lax.dot_general(a_lo, b_lo, dims, preferred_element_type=jnp.float32)
    hi = lax.dot_general(a_hi, b_hi, dims, preferred_element_type=jnp.float32)
    wide = jnp.concatenate([lo[0:128, 0:128] + hi[0:128, 0:128], lo[128:192, 0:128] + hi[192:256, 0:128]], axis=0)
    rest = jnp.concatenate(
        [lo[0:128, 128:192] + hi[0:128, 192:256], lo[128:192, 128:192] + lo[192:256, 192:256]], axis=0)
    buf[at + (0,)] = wide[0:96]
    buf[at + (1,)] = wide[96:192]
    buf[at + (2,)] = jnp.concatenate([rest[0:96], rest[96:192]], axis=1)


def move_kernel(a_ref, b_ref, o_ref, tr, pa, pb, pe, buf, sem_a, sem_b, sem_e, sem_tr, sem_o, snd, loc, out_sem):
    bat, z, row = lax.axis_index('batch'), lax.axis_index('col'), lax.axis_index('row')
    y, core = row // 2, row % 2
    size = 64 // CHUNKS

    def flip(v, n, fam):
        return jnp.where(fam == 0, v, n - v)

    def dev(col, r):
        return {'batch': bat, 'col': col, 'row': r}

    def rc(src, dst, send, recv, col, r):
        return pltpu.make_async_remote_copy(
            src_ref=src, dst_ref=dst, send_sem=send, recv_sem=recv, device_id=dev(col, r), device_id_type=MESH)

    def part(ref, c):
        return ref.at[pl.ds(c * size, size)]

    def slot(ref, s, c):
        return ref.at[s, pl.ds(c * size, size)]

    def wait_slot(ref, sem, s, c):
        rc(slot(ref, s, c), slot(ref, s, c), snd.at[0, c], sem.at[s, c], z, row).wait_recv()

    partner, across = 2 * y + 1 - core, 2 * (1 - y) + core
    diagonal = 2 * (1 - y) + 1 - core

    fam = z // 2
    blk = flip(z, 3, fam)
    home = y == fam
    k_src = flip(row, 3, fam)
    own_home = home & (row == z)
    sends_far = jnp.logical_not(home) & ((k_src == 3) | (blk == 1))

    def to_home(c):
        return rc(part(a_ref, c), slot(pa, row, c), snd.at[0, c], sem_a.at[row, c], z, z)

    def to_way(c):
        return rc(part(a_ref, c), slot(tr, blk, c), snd.at[1, c], sem_tr.at[blk, c], flip(jnp.int32(2), 3, fam), row)

    zz, ii = flip(z, 3, y), flip(row, 3, y)
    is_src = ii == zz
    inner = jnp.where(y == 0, z - 1, z + 1)
    outer = jnp.where(y == 0, z + 1, z - 1)

    def real(kk):
        return flip(jnp.int32(kk), 3, y)

    def hop(kk, c, n, col):
        k = real(kk)
        return rc(slot(pa, k, c), slot(pa, k, c), snd.at[n + kk, c], sem_a.at[k, c], col, row)

    def right(kk, c):
        return hop(kk, c, 2, outer)

    def left(kk, c):
        return hop(kk, c, 6, inner)

    goes_right = [
        (zz == 1) | ((zz == 0) & is_src),
        (zz == 1) | ((zz == 0) & is_src),
        ((zz == 1) & (ii == 0)) | ((zz == 0) & is_src),
        (zz == 0) & is_src,
    ]
    goes_left = [(zz == 1) & is_src] * 4
    goes = [goes_right[kk] | goes_left[kk] for kk in range(4)]

    ofam = 1 - y
    oz, ok = flip(z, 3, ofam), flip(row, 3, ofam)
    ways = [(oz == 2) & (ok == 3), oz == 2]

    def up(i2, c):
        return rc(slot(tr, i2, c), slot(pa, row, c), snd.at[10 + i2, c], sem_a.at[row, c], z, flip(jnp.int32(i2), 3, ofam))

    is_edge, is_inner = zz == 3, zz == 2
    not_edge = jnp.logical_not(is_edge)

    def b_far(c):
        return rc(part(b_ref, c), slot(pb, row, c), snd.at[12, c], sem_b.at[row, c], z, across)

    def b_near(c):
        return rc(part(b_ref, c), slot(pb, row, c), snd.at[13, c], sem_b.at[row, c], z, partner)

    def b_relay(c):
        return rc(slot(pb, across, c), slot(pb, across, c), snd.at[14, c], sem_b.at[across, c], z, partner)

    def e_own(c):
        return rc(part(b_ref, c), slot(pe, row, c), snd.at[13, c], sem_e.at[row, c], inner, row)

    def e_far(c):
        return rc(slot(pb, across, c), slot(pe, across, c), snd.at[14, c], sem_e.at[across, c], inner, row)

    def e_share(r, n, c):
        return rc(slot(pe, r, c), slot(pe, r, c), snd.at[n, c], sem_e.at[r, c], z, partner)

    def o_edge(c):
        return rc(buf.at[2 + c % 2], part(o_ref, c), snd.at[17, c], sem_o.at[c], outer, row)

    def o_own(c):
        return pltpu.make_async_copy(buf.at[c % 2], part(o_ref, c), out_sem.at[c % 2])

    def for_chunks(f):
        def body(c, _):
            f(c)
            return 0
        lax.fori_loop(0, CHUNKS, body, 0)

    cp_a = pltpu.make_async_copy(a_ref, pa.at[row], loc.at[0])
    cp_b = pltpu.make_async_copy(b_ref, pb.at[row], loc.at[1])

    @pl.when(own_home)
    def _():
        cp_a.start()

    cp_b.start()

    @pl.when(own_home)
    def _():
        cp_a.wait()

    cp_b.wait()

    def wait_a(kk, c):
        k = real(kk)

        @pl.when(jnp.logical_not(own_home & (k == row)))
        def _():
            wait_slot(pa, sem_a, k, c)

    forwards = [(NEAR_LAG, 0, (zz < 2) & is_src), (NEAR_LAG, 1, (zz < 2) & is_src)]
    forwards += [(CROSS_LAG, kk, (zz < 2) & is_src) for kk in (2, 3)]
    forwards += [(HOP_LAG, kk, (zz == 1) & (ii == 0)) for kk in (0, 1)]
    forwards += [(PASS_LAG, 2, (zz == 1) & (ii == 0))]

    def in_range(s, lag):
        return (s >= lag) & (s < CHUNKS + lag)

    b_lag = jnp.where(is_inner, INNER_LAG, B_LAG)
    sum_lag = jnp.where(is_inner, INNER_LAG + 1, SUM_LAG)

    def step(s, _):
        for lag, kk, who in forwards:
            @pl.when(in_range(s, lag) & who)
            def _():
                c = s - lag
                wait_a(kk, c)

                @pl.when(goes_right[kk])
                def _():
                    right(kk, c).start()

                @pl.when(goes_left[kk])
                def _():
                    left(kk, c).start()

        @pl.when(s < CHUNKS)
        def _():
            @pl.when(jnp.logical_not(own_home))
            def _():
                to_home(s).start()

            @pl.when(sends_far)
            def _():
                to_way(s).start()

            b_far(s).start()

            @pl.when(is_edge)
            def _():
                e_own(s).start()

            @pl.when(not_edge)
            def _():
                b_near(s).start()

        @pl.when(in_range(s, WAY_LAG))
        def _():
            c = s - WAY_LAG
            for i2 in range(2):
                @pl.when(ways[i2])
                def _():
                    wait_slot(tr, sem_tr, i2, c)
                    up(i2, c).start()

        @pl.when(in_range(s, EDGE_LAG) & is_edge)
        def _():
            c = s - EDGE_LAG
            wait_slot(pb, sem_b, across, c)
            e_far(c).start()

        @pl.when(in_range(s, b_lag) & not_edge)
        def _():
            c = s - b_lag
            wait_slot(pb, sem_b, across, c)
            b_relay(c).start()

        for r, n in ((row, 15), (across, 16)):
            @pl.when(in_range(s, INNER_LAG) & is_inner)
            def _():
                c = s - INNER_LAG
                wait_slot(pe, sem_e, r, c)
                e_share(r, n, c).start()

        @pl.when(in_range(s, sum_lag) & not_edge)
        def _():
            c = s - sum_lag
            for r in (partner, diagonal):
                wait_slot(pb, sem_b, r, c)
            for kk in range(4):
                @pl.when(jnp.logical_not(goes[kk]))
                def _():
                    wait_a(kk, c)

            @pl.when(is_inner)
            def _():
                for r in (partner, diagonal):
                    wait_slot(pe, sem_e, r, c)

                @pl.when(c >= 2)
                def _():
                    o_edge(c - 2).wait_send()

                def edge(h, _):
                    channel_sum(pa, pe, c * size + h, buf, (2 + c % 2, h))
                    return 0

                lax.fori_loop(0, size, edge, 0)
                o_edge(c).start()

            @pl.when(c >= 2)
            def _():
                o_own(c - 2).wait()

            def own(h, _):
                channel_sum(pa, pb, c * size + h, buf, (c % 2, h))
                return 0

            lax.fori_loop(0, size, own, 0)
            o_own(c).start()
        return 0

    lax.fori_loop(0, CHUNKS + max(SUM_LAG, INNER_LAG + 1), step, 0)

    @pl.when(not_edge)
    def _():
        for c in range(CHUNKS - 2, CHUNKS):
            o_own(c).wait()

    @pl.when(is_inner)
    def _():
        for c in range(CHUNKS - 2, CHUNKS):
            o_edge(c).wait_send()

    def drain(c):
        @pl.when(jnp.logical_not(own_home))
        def _():
            to_home(c).wait_send()

        @pl.when(sends_far)
        def _():
            to_way(c).wait_send()

        b_far(c).wait_send()

        @pl.when(not_edge)
        def _():
            b_near(c).wait_send()
            b_relay(c).wait_send()

        @pl.when(is_edge)
        def _():
            e_own(c).wait_send()
            e_far(c).wait_send()
            rc(buf.at[0], part(o_ref, c), snd.at[0, c], sem_o.at[c], z, row).wait_recv()

        @pl.when(is_inner)
        def _():
            e_share(row, 15, c).wait_send()
            e_share(across, 16, c).wait_send()

        for kk in range(4):
            @pl.when(goes_right[kk])
            def _():
                right(kk, c).wait_send()

            @pl.when(goes_left[kk])
            def _():
                left(kk, c).wait_send()

        for i2 in range(2):
            @pl.when(ways[i2])
            def _():
                up(i2, c).wait_send()

    for_chunks(drain)


def move(a, b):
    tile = (64, 3, 96, 128)
    any_spec = pl.BlockSpec(memory_space=pltpu.HBM)
    o, _ = pl.pallas_call(
        move_kernel,
        out_shape=[jax.ShapeDtypeStruct(tile, jnp.float32), jax.ShapeDtypeStruct((2,) + tile, jnp.bfloat16)],
        in_specs=[any_spec] * 2,
        out_specs=[any_spec] * 2,
        scratch_shapes=[pltpu.VMEM((4,) + tile, jnp.bfloat16)] * 3 + [
            pltpu.VMEM((4, 64 // CHUNKS, 3, 96, 128), jnp.float32),
            pltpu.SemaphoreType.DMA((4, CHUNKS)),
            pltpu.SemaphoreType.DMA((4, CHUNKS)),
            pltpu.SemaphoreType.DMA((4, CHUNKS)),
            pltpu.SemaphoreType.DMA((2, CHUNKS)),
            pltpu.SemaphoreType.DMA((CHUNKS,)),
            pltpu.SemaphoreType.DMA((18, CHUNKS)),
            pltpu.SemaphoreType.DMA((2,)),
            pltpu.SemaphoreType.DMA((2,)),
        ],
        compiler_params=pltpu.CompilerParams(has_side_effects=True, vmem_limit_bytes=67043328),
    )(a, b)
    return o


def finish_kernel(o_ref, z_ref, gin_ref, gout_ref, wg_ref, wo_ref, out_ref, gi_ref, go_ref, wg4_ref, wo8_ref):
    @pl.when(pl.program_id(0) == 0)
    def _():
        gi_ref[...] = jnp.broadcast_to(column(ids((64, 64), 0) == ids((64, 64), 1), gin_ref[...]), (64, 384))
        go_ref[...] = jnp.broadcast_to(column(ids((512, 64), 0) // 8 == ids((512, 64), 1), gout_ref[...]), (512, 128))
        t = pick(ids((256, 64), 0) % 64 == ids((256, 64), 1), wg_ref[...])
        t = jnp.concatenate([t] * 4, axis=1)
        same = ids((256, 256), 0) // 64 == ids((256, 256), 1) // 64
        wg4_ref[...] = jnp.where(same, t, 0.0).astype(jnp.bfloat16)
        t = pick(ids((512, 64), 0) % 64 == ids((512, 64), 1), wo_ref[...]).astype(jnp.bfloat16)
        wide = (ids((64, 512), 1) // 8 == ids((64, 512), 0)).astype(jnp.bfloat16)
        t = jnp.dot(t, wide, preferred_element_type=jnp.float32)
        same = ids((512, 512), 0) // 64 == ids((512, 512), 1) % 8
        wo8_ref[...] = jnp.where(same, t, 0.0).astype(jnp.bfloat16)

    for q in range(2):
        rows = slice(8 * q, 8 * q + 8)
        normed = []
        for sec in range(3):
            v = norm_channels(o_ref[:, sec, rows], 1.0, 0).reshape(512, 128) * go_ref[...]
            normed.append(v.astype(jnp.bfloat16))
        upd = jnp.dot(wo8_ref[...], jnp.concatenate(normed, axis=1), preferred_element_type=jnp.float32)
        z = lanes(z_ref[0, rows], z_ref[1, rows]).astype(jnp.float32)
        x = norm_channels(z, gi_ref[...][None], 1).astype(jnp.bfloat16).reshape(512, 384)
        gate = jnp.concatenate(
            [jnp.dot(wg4_ref[...], x[256 * s:256 * s + 256], preferred_element_type=jnp.float32) for s in range(2)], axis=0)
        res = (z.reshape(512, 384) + sigmoid(gate) * upd).astype(jnp.bfloat16).reshape(8, 64, 384)
        out_ref[0, rows] = jnp.concatenate([res[:, :, :128], res[:, :, 256:320]], axis=2)
        out_ref[1, rows] = jnp.concatenate([res[:, :, 128:256], res[:, :, 320:]], axis=2)


def finish(o, z, gin, gout, w_g, w_o):
    rows = pl.BlockSpec((2, 16, 64, 192), lambda i: (0, i, 0, 0))
    full = lambda i: (0, 0)
    out = pl.pallas_call(
        finish_kernel,
        grid=(6,),
        out_shape=jax.ShapeDtypeStruct((2, 96, 64, 192), jnp.bfloat16),
        in_specs=[
            pl.BlockSpec((64, 3, 16, 128), lambda i: (0, 0, i, 0)),
            rows,
            pl.BlockSpec((1, 64), full),
            pl.BlockSpec((1, 64), full),
            pl.BlockSpec((64, 64), full),
            pl.BlockSpec((64, 64), full),
        ],
        out_specs=rows,
        scratch_shapes=[
            pltpu.VMEM((64, 384), jnp.float32),
            pltpu.VMEM((512, 128), jnp.float32),
            pltpu.VMEM((256, 256), jnp.bfloat16),
            pltpu.VMEM((512, 512), jnp.bfloat16),
        ],
        compiler_params=pltpu.CompilerParams(vmem_limit_bytes=60 * 1024 * 1024),
    )(o, z.reshape(2, 96, 64, 192), gin, gout, w_g, w_o)
    return out.reshape(192, 64, 192)


def solution(mesh):
    tile_spec = P(('batch', 'row'), 'col', None)
    mask_spec = P(('batch', 'row'), 'col')
    replicated = P()

    def local_step(pair, mask, gin, w_l, w_lg, w_r, w_rg, w_g, gout, w_o):
        z = jnp.transpose(pair, (0, 2, 1))
        a, b = project(z, mask, gin[None], w_l, w_lg, w_r, w_rg)
        o = move(a, b)
        out = finish(o, z, gin[None], gout[None], w_g, w_o)
        return jnp.transpose(out, (0, 2, 1))

    return jax.shard_map(local_step, mesh=mesh, in_specs=(tile_spec, mask_spec) + (replicated,) * 8, out_specs=tile_spec, check_vma=False)
```
